32 devices in a mesh: own: 8 (over z, x), rep: 4 (over y, core).
Axes of the slice: x: 2, y: 2, z: 4, core: 2. Of those that a mesh axis runs over, the one named last changes fastest.
Arguments:
- block_pool: bfloat16 [2048, 64, 576], P(('own', 'rep')), may hold values from -16 to 16
- sel_index: int32 [1024], P(('own', 'rep')), may hold values from 0 to 63
- sel_layer: int32 [1024], P(('own', 'rep')), may hold values from 0 to 3, as said below
- counts: int32 [32], P(('own', 'rep')), may hold values from 8 to 32, as said below
Outputs:
- quant_codes: bfloat16 [8, 4, 8, 8, 18432], P('own', 'rep')
- quant_steps: float32 [8, 288], P('own')
- clip_error: float32 [8, 288], P('own')
The draws below stay inside these ranges and needn't reach their ends.
Inputs may be any that keep to these rules, and one draw needn't show every extreme that they name: `sel_layer`: among the 32 entries of one device, at most 8 name any one layer; the first 8 entries of every device all name one and the same layer. `counts`: some device has all 32 entries live.
All inputs are finite; a program needn't handle non-finite values.
Results may differ from the reference program's by a relative error of at most 0.001.
Values may be sent and summed in bfloat16 or wider, within the bound.
A program may use at most 128 MiB of HBM per device.

```python
import math
import jax
import jax.numpy as jnp
from jax import lax

LATENT = 576
TOKB = 64
SLICES = 2
CAP = 8
POOL_DEV = 64
SEL_DEV = 32
LAYERS = 4
HALF = 288
SEL_ALL = 1024
N_OWN = 8
N_REP = 4


def draw_block_pool(key, part):
    base_key = jax.random.fold_in(key, 11)
    key_chan, key_base, key_rows = jax.random.split(base_key, 3)
    shape = (N_OWN * N_REP * POOL_DEV, TOKB, LATENT)
    channel = jnp.exp(jax.random.uniform(key_chan, (LATENT,), jnp.float32, math.log(0.3), math.log(3.0)))
    base = jnp.clip(jax.random.normal(key_base, shape, jnp.float32), -5.0, 5.0)
    row_scale = jnp.ones((shape[0], 1, 1), jnp.float32)
    return (base * channel * row_scale).astype(jnp.bfloat16)


def draw_sel_layer(key, part):
    devices = N_OWN * N_REP
    base_key = jax.random.fold_in(key, 31)
    key_star, key_perm = jax.random.split(base_key, 2)
    star_layer = jax.random.randint(key_star, (), 0, LAYERS)
    items = jnp.arange((LAYERS - 1) * CAP, dtype=jnp.int32) // CAP
    device_keys = jax.random.split(key_perm, devices)

    def per_device(device_key):
        shuffled = jax.random.permutation(device_key, items)[:SEL_DEV - CAP]
        others = (star_layer + 1 + shuffled) % LAYERS
        front = jnp.full((CAP,), star_layer, jnp.int32)
        return jnp.concatenate([front, others.astype(jnp.int32)])
    return jax.vmap(per_device)(device_keys).reshape(-1).astype(jnp.int32)


def draw_counts(key, part):
    devices = N_OWN * N_REP
    base_key = jax.random.fold_in(key, 21)
    key_low, key_full, key_first = jax.random.split(base_key, 3)
    lower = jax.random.randint(key_low, (devices,), CAP, CAP + (SEL_DEV - CAP) // 3 + 1)
    full_mask = jax.random.randint(key_full, (devices,), 0, 8) == 0
    first_full = jax.random.randint(key_first, (), 0, devices)
    full_mask = full_mask | (jnp.arange(devices) == first_full)
    return jnp.where(full_mask, SEL_DEV, lower).astype(jnp.int32)


def touch_ends(drawn, stream_key, low, high):
    index_at = [jax.random.randint(jax.random.fold_in(stream_key, axis), (), 0, length) for axis, length in enumerate(drawn.shape)]
    main_axis = drawn.shape.index(max(drawn.shape))
    neighbour = index_at[:main_axis] + [(index_at[main_axis] + 1) % drawn.shape[main_axis]] + index_at[main_axis + 1:]
    return drawn.at[tuple(index_at)].set(low).at[tuple(neighbour)].set(high)


def setup_inputs(seed: int = 0) -> dict:
    seeds = jax.random.split(jax.random.key(seed), 5)
    return {
        "block_pool": draw_block_pool(jax.random.fold_in(seeds[4], 71), 0),
        "sel_index": touch_ends(jax.random.randint(seeds[1], (SEL_ALL,), 0, POOL_DEV), jax.random.fold_in(seeds[1], 1), 0, POOL_DEV - 1).astype(jnp.int32),
        "sel_layer": draw_sel_layer(jax.random.fold_in(seeds[4], 71), 0),
        "counts": draw_counts(jax.random.fold_in(seeds[4], 71), 0),
    }


headroom = 0.5


def slot_table(index_row, layer_row, live_count, group_layer, capacity):
    n_select = index_row.shape[0]
    is_live = jnp.arange(n_select) < live_count
    matches = (layer_row[None, :] == group_layer[:, None]) & is_live[None, :]
    ranking = jnp.cumsum(matches.astype(jnp.int32), axis=1) - 1
    slot_hit = matches[:, None, :] & (ranking[:, None, :] == jnp.arange(capacity)[None, :, None])
    chosen = jnp.sum(jnp.where(slot_hit, index_row[None, None, :], 0), axis=2).astype(jnp.int32)
    filled = jnp.any(slot_hit, axis=2)
    return chosen, filled


def reference(block_pool, sel_index, sel_layer, counts):
    devices = N_OWN * N_REP
    group_layer = (jnp.arange(N_OWN) // SLICES).astype(jnp.int32)
    index_rows = sel_index.reshape(devices, SEL_DEV)
    layer_rows = sel_layer.reshape(devices, SEL_DEV)
    chosen, filled = jax.vmap(lambda a, b, c: slot_table(a, b, c, group_layer, CAP))(index_rows, layer_rows, counts)
    pools = block_pool.reshape(devices, POOL_DEV, TOKB, SLICES, HALF)
    device_ids = jnp.arange(devices)[:, None]
    denominator = float(N_OWN * N_REP * CAP * TOKB)

    def one_group(group):
        slice_of = group % SLICES
        picked = jnp.take(chosen, group, axis=1)
        keep_mask = jnp.take(filled, group, axis=1)
        blocks = pools[device_ids, picked, :, slice_of]
        blocks = jnp.where(keep_mask[:, :, None, None], blocks, jnp.zeros((), blocks.dtype))
        values = blocks.astype(jnp.float32)
        peak_abs = jnp.max(jnp.abs(values), axis=(0, 1, 2))
        step_size = headroom * jnp.maximum(peak_abs, 1.0) / 127.0
        encoded = jnp.clip(values / step_size, -127.0, 127.0).astype(jnp.bfloat16)
        encoded = lax.optimization_barrier(encoded)
        decoded = encoded.astype(jnp.float32) * step_size
        sq_error = jnp.sum((values - decoded) ** 2, axis=(0, 1, 2))
        error_out = sq_error / (step_size * step_size * denominator)
        codes_out = encoded.reshape(N_OWN, N_REP, CAP, TOKB * HALF).transpose(1, 0, 2, 3)
        return codes_out, step_size, error_out

    quant_codes, quant_steps, clip_error = lax.map(one_group, jnp.arange(N_OWN))
    return quant_codes, quant_steps, clip_error
```

```python
import functools
import math

import jax
import jax.numpy as jnp
from jax import lax
from jax.experimental import pallas as pl
from jax.experimental.pallas import tpu as pltpu
from jax.sharding import PartitionSpec as P

SLICES = 2
LANES = 128
headroom = 0.5


def ring_place(layer, layers):
    odd = layer % 2
    return odd * ((layer + 1) // 2) + (1 - odd) * lax.rem(layers - layer // 2, layers)


def ring_layer(place, layers):
    near = jnp.maximum(2 * place - 1, 0)
    return jnp.where(place <= layers // 2, near, 2 * (layers - place))


def partner_layer(my_layer, layers, k):
    return ring_layer(lax.rem(ring_place(my_layer, layers) + k, layers), layers)


def fill_slots(live, index_row, layer_row, table, layers, cap, empty):
    n_select = index_row.shape[1]
    is_live = lax.broadcasted_iota(jnp.int32, (1, n_select), 1) < live
    before = lax.broadcasted_iota(jnp.int32, (n_select, n_select), 0)
    after = lax.broadcasted_iota(jnp.int32, (n_select, n_select), 1)
    earlier = jnp.where(before < after, 1.0, 0.0)
    wanted = lax.broadcasted_iota(jnp.int32, (layers, n_select), 0)
    matches = jnp.where((layer_row == wanted) & is_live, 1.0, 0.0)
    ranking = jnp.dot(matches, earlier, preferred_element_type=jnp.float32)
    slot = lax.broadcasted_iota(jnp.int32, (cap, n_select), 0).astype(jnp.float32)
    shifted = index_row.astype(jnp.float32) - float(empty)
    for layer in range(layers):
        hit = (ranking[layer:layer + 1] == slot) & (matches[layer:layer + 1] > 0.5)
        found = jnp.sum(jnp.where(hit, shifted, 0.0), axis=1, keepdims=True) + float(empty)
        table[layer * cap:(layer + 1) * cap, :] = jnp.broadcast_to(found, (cap, LANES)).astype(jnp.int32)


def kernel(own_n, rep_n, cap, live_hbm, index_hbm, layer_hbm, pool_ref, codes_ref, steps_ref, err_ref,
           live_v, index_v, layer_v, table, slots, pool_v, stage, send, recv,
           pk_send, pk_recv, pk_mine, pk_rep, st_mine, st_recv, pe_send, pe_recv, er_mine, er_rep,
           small_sem, table_sem, pool_sem, ssem, rsem, pssem, prsem, rpssem, rprsem, tssem, trsem,
           essem, ersem, ressem, rersem):
    rows, tokens, width = pool_ref.shape
    half = width // SLICES
    group = LANES // math.gcd(half, LANES)
    period = group * half
    loops = tokens // group
    layers = own_n // SLICES
    me = lax.axis_index("own")
    rep = lax.axis_index("rep")
    my_layer = me // SLICES
    my_slice = me % SLICES
    tiles = stage.shape[0]
    denominator = float(own_n * rep_n * cap * tokens)
    pieces = pool_sem.shape[0]
    per_piece = rows // pieces
    f32 = jnp.float32

    barrier = pltpu.get_barrier_semaphore()
    for k in range(1, own_n):
        pl.semaphore_signal(barrier, inc=1, device_id={"own": lax.rem(me + k, own_n)},
                            device_id_type=pl.DeviceIdType.MESH)
    for k in range(1, rep_n):
        pl.semaphore_signal(barrier, inc=1, device_id={"rep": lax.rem(rep + k, rep_n)},
                            device_id_type=pl.DeviceIdType.MESH)

    smalls = [pltpu.make_async_copy(a, b, small_sem.at[i])
              for i, (a, b) in enumerate(((live_hbm, live_v), (index_hbm, index_v), (layer_hbm, layer_v)))]
    for small in smalls:
        small.start()
    loads = [
        pltpu.make_async_copy(
            pool_ref.at[pl.ds(p * per_piece, per_piece)],
            pool_v.at[pl.ds(p * per_piece, per_piece)],
            pool_sem.at[p],
        )
        for p in range(pieces)
    ]
    for load in loads:
        load.start()

    pool_v[rows] = jnp.zeros((tokens, width), pool_v.dtype)
    for small in smalls:
        small.wait()
    fill_slots(live_v[...], index_v[...], layer_v[...], table, layers, cap, rows)
    to_scalars = pltpu.make_async_copy(table, slots, table_sem)
    to_scalars.start()
    to_scalars.wait()
    for load in loads:
        load.wait()

    def row_of(slot):
        return jnp.minimum(jnp.maximum(slots[slot, 0], 0), rows)

    def layer_peak(layer, carry):
        best = jnp.zeros((tokens, width), pool_v.dtype)
        for c in range(cap):
            best = jnp.maximum(best, jnp.abs(pool_v[row_of(layer * cap + c)]))
        top = jnp.max(best.astype(f32), axis=0, keepdims=True)
        for part in range(SLICES):
            pk_send[layer * SLICES + part] = top[:, part * half:(part + 1) * half]
        return carry

    def own_copy(src, dst, s_sem, r_sem, peer):
        return pltpu.make_async_remote_copy(
            src_ref=src, dst_ref=dst, send_sem=s_sem, recv_sem=r_sem,
            device_id={"own": peer}, device_id_type=pl.DeviceIdType.MESH)

    def rep_copy(mine, table, s_sem, r_sem, peer, landing):
        return pltpu.make_async_remote_copy(
            src_ref=mine, dst_ref=table.at[landing],
            send_sem=s_sem.at[peer], recv_sem=r_sem.at[landing],
            device_id={"rep": peer}, device_id_type=pl.DeviceIdType.MESH)

    def peak_copy(peer, landing):
        return own_copy(pk_send.at[peer], pk_recv.at[landing], pssem.at[peer], prsem.at[landing], peer)

    def step_copy(peer, landing):
        return own_copy(st_mine, st_recv.at[landing], tssem.at[peer], trsem.at[landing], peer)

    def part_error_copy(peer, landing):
        return own_copy(pe_send.at[peer], pe_recv.at[landing], essem.at[peer], ersem.at[landing], peer)

    quarter = loops // 4
    first, middle, rest = (0, quarter, 0), (quarter, loops - 2 * quarter, 1), (loops - quarter, quarter, 2)
    all_cols = (0, loops, 0)

    def block_copy(peer, landing, cols, into):
        lanes = pl.ds(cols[0] * period, cols[1] * period)
        to = into.at[0, 0] if len(into.shape) == 5 else into
        return own_copy(send.at[peer, :, lanes], to.at[landing, :, lanes],
                        ssem.at[peer, cols[2]], rsem.at[landing, cols[2]], peer)

    def flatten_layer(layer, cols):
        start, count, _ = cols
        t0, t1 = start * group, (start + count) * group
        for c in range(cap):
            block = pool_v[row_of(layer * cap + c), t0:t1, :].astype(f32)
            for q in range(tiles):
                lo, hi = q * LANES, min(width, (q + 1) * LANES)
                stage[q, c * tokens + t0:c * tokens + t1, 0:hi - lo] = block[:, lo:hi]

        def flatten(i, carry):
            rows_of = [
                jnp.concatenate(
                    [stage[q, pl.ds(i * group + j, cap, stride=tokens), :] for q in range(tiles)], axis=1)
                for j in range(group)
            ]
            for part in range(SLICES):
                joined = jnp.concatenate([r[:, part * half:(part + 1) * half] for r in rows_of], axis=1)
                at = pl.multiple_of(i * period, period)
                send[layer * SLICES + part, :, pl.ds(at, period)] = joined.astype(send.dtype)
            return carry

        lax.fori_loop(start, start + count, flatten, 0)

    def owner(layer, part):
        return layer * SLICES + lax.rem(my_slice + part, SLICES)

    across_first = list(range(1, SLICES)) + [0]
    order = [k for k in range(1, layers) if k != layers // 2]
    last = partner_layer(my_layer, layers, layers // 2)
    to_layer = [partner_layer(my_layer, layers, k) for k in order]
    from_layer = [partner_layer(my_layer, layers, layers - k) for k in order]

    def send_blocks(layer, cols):
        for part in across_first:
            block_copy(owner(layer, part), me, cols, recv).start()

    lax.fori_loop(0, layers, layer_peak, 0)
    flatten_layer(to_layer[0], first)
    pl.semaphore_wait(barrier, own_n - 1 + rep_n - 1)
    for k in range(1, own_n):
        peer = lax.rem(me + k, own_n)
        peak_copy(peer, me).start()
    send_blocks(to_layer[0], first)
    flatten_layer(to_layer[0], middle)
    send_blocks(to_layer[0], middle)
    flatten_layer(to_layer[0], rest)

    best = pk_send[me]
    for k in range(1, own_n):
        src = lax.rem(me + k, own_n)
        peak_copy(src, src).wait_recv()
        best = jnp.maximum(best, pk_recv[src])
    pk_mine[...] = best
    for k in range(1, rep_n):
        rep_copy(pk_mine, pk_rep, rpssem, rprsem, lax.rem(rep + k, rep_n), rep).start()
    flatten_layer(last, all_cols)
    for k in range(1, rep_n):
        src = lax.rem(rep + k, rep_n)
        rep_copy(pk_mine, pk_rep, rpssem, rprsem, src, src).wait_recv()
        best = jnp.maximum(best, pk_rep[src])

    step = headroom * jnp.maximum(best, 1.0) / 127.0
    steps_ref[...] = step
    st_mine[...] = step
    for part in across_first:
        step_copy(owner(last, part), me).start()
    send_blocks(to_layer[0], rest)
    for i, layer in enumerate(to_layer[1:]):
        flatten_layer(layer, all_cols)
        send_blocks(layer, all_cols)
    flatten_layer(my_layer, all_cols)
    for part in range(1, SLICES):
        block_copy(owner(my_layer, part), me, all_cols, recv).start()

    def wide(row):
        return jnp.broadcast_to(jnp.concatenate([row] * group, axis=1), (cap, period))

    def encode(source, target, src, one_step, total):
        step_wide = wide(one_step)
        inv_wide = wide(1.0 / one_step)

        def one(i, total):
            lanes = pl.ds(pl.multiple_of(i * period, period), period)
            x = source[src, :, lanes].astype(f32)
            y = jnp.clip(x * inv_wide, -127.0, 127.0).astype(codes_ref.dtype)
            target[src, :, lanes] = y
            diff = x - y.astype(f32) * step_wide
            return total + diff * diff
        return lax.fori_loop(0, loops, one, total)

    def fold(total):
        row = jnp.sum(total, axis=0, keepdims=True)
        folded = row[:, :half]
        for j in range(1, group):
            folded = folded + row[:, j * half:(j + 1) * half]
        return folded

    zero = jnp.zeros((cap, period), f32)
    codes_at = codes_ref.at[0, 0]
    total = encode(send, codes_at, me, step, zero)

    for part in across_first:
        peer = owner(last, part)
        step_copy(peer, peer).wait_recv()
        pe_send[peer] = fold(encode(send, send, peer, st_recv[peer], zero))
        part_error_copy(peer, me).start()
        block_copy(peer, me, all_cols, codes_ref).start()

    for part in across_first:
        src = owner(from_layer[0], part)
        for cols in (first, middle, rest):
            block_copy(src, src, cols, recv).wait_recv()
        total = encode(recv, codes_at, src, step, total)
    for part in range(1, SLICES):
        src = owner(my_layer, part)
        block_copy(src, src, all_cols, recv).wait_recv()
        total = encode(recv, codes_at, src, step, total)
    for i, layer in enumerate(from_layer[1:]):
        for part in across_first:
            src = owner(layer, part)
            block_copy(src, src, all_cols, recv).wait_recv()
            total = encode(recv, codes_at, src, step, total)

    mine = fold(total)
    for part in across_first:
        src = owner(last, part)
        part_error_copy(src, src).wait_recv()
        mine = mine + pe_recv[src]
    er_mine[...] = mine
    for k in range(1, rep_n):
        rep_copy(er_mine, er_rep, ressem, rersem, lax.rem(rep + k, rep_n), rep).start()
    er_rep[rep] = mine
    for k in range(1, rep_n):
        src = lax.rem(rep + k, rep_n)
        rep_copy(er_mine, er_rep, ressem, rersem, src, src).wait_recv()
    whole = er_rep[0]
    for k in range(1, rep_n):
        whole = whole + er_rep[k]
    err_ref[...] = whole / (step * step * denominator)

    for k in range(1, own_n):
        peak_copy(lax.rem(me + k, own_n), me).wait_send()
    for k in range(1, rep_n):
        peer = lax.rem(rep + k, rep_n)
        rep_copy(pk_mine, pk_rep, rpssem, rprsem, peer, rep).wait_send()
        rep_copy(er_mine, er_rep, ressem, rersem, peer, rep).wait_send()
    for part in across_first:
        step_copy(owner(last, part), me).wait_send()
        part_error_copy(owner(last, part), me).wait_send()
        for cols in (first, middle, rest):
            block_copy(owner(to_layer[0], part), me, cols, recv).wait_send()
        for layer in to_layer[1:]:
            block_copy(owner(layer, part), me, all_cols, recv).wait_send()
    for part in range(1, SLICES):
        block_copy(owner(my_layer, part), me, all_cols, recv).wait_send()
    for part in across_first:
        peer = owner(last, part)
        block_copy(peer, me, all_cols, codes_ref).wait_send()
        block_copy(peer, peer, all_cols, codes_ref).wait_recv()


def write_out(codes_v, steps_v, err_v, codes_ref, steps_ref, err_ref, sems):
    own_n = codes_v.shape[2]
    moves = [pltpu.make_async_copy(codes_v.at[0, 0, src], codes_ref.at[0, 0, src], sems.at[src])
             for src in range(own_n)]
    moves.append(pltpu.make_async_copy(steps_v, steps_ref, sems.at[own_n]))
    moves.append(pltpu.make_async_copy(err_v, err_ref, sems.at[own_n + 1]))
    for move in moves:
        move.start()
    for move in moves:
        move.wait()


def body(block_pool, sel_index, sel_layer, counts):
    own_n = lax.axis_size("own")
    rep_n = lax.axis_size("rep")
    cap = sel_index.shape[0] // 4
    rows, tokens, width = block_pool.shape
    n_select = sel_index.shape[0]
    half = width // SLICES
    flat = tokens * half
    layers = own_n // SLICES
    f32, i32 = jnp.float32, jnp.int32
    dma = pltpu.SemaphoreType.DMA
    dtype = block_pool.dtype
    hbm = pl.BlockSpec(memory_space=pltpu.HBM)
    vmem = pl.BlockSpec(memory_space=pltpu.VMEM)
    codes, steps, err = pl.pallas_call(
        functools.partial(kernel, own_n, rep_n, cap),
        out_shape=(
            pltpu.VMEM((1, 1, own_n, cap, flat), dtype),
            pltpu.VMEM((1, half), f32),
            pltpu.VMEM((1, half), f32),
        ),
        in_specs=[hbm] * 4,
        out_specs=(vmem,) * 3,
        scratch_shapes=[
            pltpu.VMEM((1, 1), i32), pltpu.VMEM((1, n_select), i32), pltpu.VMEM((1, n_select), i32),
            pltpu.VMEM((layers * cap, LANES), i32),
            pltpu.SMEM((layers * cap, LANES), i32),
            pltpu.VMEM((rows + 1, tokens, width), dtype),
            pltpu.VMEM((pl.cdiv(width, LANES), cap * tokens, LANES), f32),
            pltpu.VMEM((own_n, cap, flat), dtype),
            pltpu.VMEM((own_n, cap, flat), dtype),
            pltpu.VMEM((own_n, 1, half), f32), pltpu.VMEM((own_n, 1, half), f32),
            pltpu.VMEM((1, half), f32), pltpu.VMEM((rep_n, 1, half), f32),
            pltpu.VMEM((1, half), f32), pltpu.VMEM((own_n, 1, half), f32),
            pltpu.VMEM((own_n, 1, half), f32), pltpu.VMEM((own_n, 1, half), f32),
            pltpu.VMEM((1, half), f32), pltpu.VMEM((rep_n, 1, half), f32),
            dma((3,)), dma, dma((8,)),
            dma((own_n, 3)), dma((own_n, 3)), dma((own_n,)), dma((own_n,)),
            dma((rep_n,)), dma((rep_n,)), dma((own_n,)), dma((own_n,)),
            dma((own_n,)), dma((own_n,)), dma((rep_n,)), dma((rep_n,)),
        ],
        compiler_params=pltpu.CompilerParams(
            collective_id=0, has_side_effects=True, vmem_limit_bytes=(63 * 1024 * 1024 - own_n * cap * flat * 2)),
        name="latent_code",
    )(counts[None], sel_index[None], sel_layer[None], block_pool)
    return pl.pallas_call(
        write_out,
        out_shape=tuple(jax.ShapeDtypeStruct(x.shape, x.dtype) for x in (codes, steps, err)),
        in_specs=[vmem] * 3,
        out_specs=(hbm, hbm, hbm),
        scratch_shapes=[dma((own_n + 2,))],
        compiler_params=pltpu.CompilerParams(vmem_limit_bytes=4 * 1024 * 1024),
        name="write_out",
    )(codes, steps, err)


def solution(mesh):
    return jax.shard_map(
        body,
        mesh=mesh,
        in_specs=(
            P(("own", "rep"), None, None),
            P(("own", "rep")),
            P(("own", "rep")),
            P(("own", "rep")),
        ),
        out_specs=(P("own", "rep", None, None, None), P("own", None), P("own", None)),
        check_vma=False,
    )
```

```python
import functools
import math

import jax
import jax.numpy as jnp
from jax import lax
from jax.experimental import pallas as pl
from jax.experimental.pallas import tpu as pltpu
from jax.sharding import PartitionSpec as P

SLICES = 2
LANES = 128
PIECES = 8
headroom = 0.5


def ring_place(layer, layers):
    odd = layer % 2
    return odd * ((layer + 1) // 2) + (1 - odd) * lax.rem(layers - layer // 2, layers)


def ring_layer(place, layers):
    near = jnp.maximum(2 * place - 1, 0)
    return jnp.where(place <= layers // 2, near, 2 * (layers - place))


def partner_layer(my_layer, layers, k):
    return ring_layer(lax.rem(ring_place(my_layer, layers) + k, layers), layers)


def fill_slots(live, index_row, layer_row, table, layers, cap, empty):
    n_select = index_row.shape[1]
    is_live = lax.broadcasted_iota(jnp.int32, (1, n_select), 1) < live
    before = lax.broadcasted_iota(jnp.int32, (n_select, n_select), 0)
    after = lax.broadcasted_iota(jnp.int32, (n_select, n_select), 1)
    earlier = jnp.where(before < after, 1.0, 0.0)
    wanted = lax.broadcasted_iota(jnp.int32, (layers, n_select), 0)
    matches = jnp.where((layer_row == wanted) & is_live, 1.0, 0.0)
    ranking = jnp.dot(matches, earlier, preferred_element_type=jnp.float32)
    slot = lax.broadcasted_iota(jnp.int32, (cap, n_select), 0).astype(jnp.float32)
    shifted = index_row.astype(jnp.float32) - float(empty)
    for layer in range(layers):
        hit = (ranking[layer:layer + 1] == slot) & (matches[layer:layer + 1] > 0.5)
        found = jnp.sum(jnp.where(hit, shifted, 0.0), axis=1, keepdims=True) + float(empty)
        table[layer * cap:(layer + 1) * cap, :] = jnp.broadcast_to(found, (cap, LANES)).astype(jnp.int32)


def kernel(own_n, rep_n, cap, live_ref, index_hbm, layer_hbm, pool_ref, codes_ref, steps_ref, err_ref,
           sel_v, table, slots, pool_a, pool_b, stage, send, recv, pk_send, pk_recv, pk_rep,
           st_recv, pe_send, pe_recv, er_rep, mine,
           sel_sem, table_sem, pool_sem, send_sem, recv_sem, small_send, small_recv):
    rows, tokens, width = pool_ref.shape
    half = width // SLICES
    group = LANES // math.gcd(half, LANES)
    period = group * half
    loops = tokens // group
    layers = own_n // SLICES
    me = lax.axis_index("own")
    rep = lax.axis_index("rep")
    my_layer = me // SLICES
    my_slice = me % SLICES
    tiles = stage.shape[0]
    denominator = float(own_n * rep_n * cap * tokens)
    f32 = jnp.float32
    early = pool_a.shape[1]

    sels = [pltpu.make_async_copy(index_hbm, sel_v.at[0], sel_sem),
            pltpu.make_async_copy(layer_hbm, sel_v.at[1], sel_sem)]
    for sel in sels:
        sel.start()
    barrier = pltpu.get_barrier_semaphore()
    for k in range(1, own_n):
        pl.semaphore_signal(barrier, inc=1, device_id={"own": lax.rem(me + k, own_n)},
                            device_id_type=pl.DeviceIdType.MESH)
    for k in range(1, rep_n):
        pl.semaphore_signal(barrier, inc=1, device_id={"rep": lax.rem(rep + k, rep_n)},
                            device_id_type=pl.DeviceIdType.MESH)
    for pool, start, sem in ((pool_a, 0, pool_sem.at[0]), (pool_b, early, pool_sem.at[1])):
        for p in range(PIECES):
            here = pl.ds(p * (rows // PIECES), rows // PIECES)
            pltpu.make_async_copy(pool_ref.at[here, start:start + pool.shape[1]], pool.at[here], sem).start()

    def load_wait(pool, sem):
        pltpu.make_async_copy(pool_ref.at[:, 0:pool.shape[1]], pool.at[pl.ds(0, rows)], sem).wait()

    pool_a[rows] = jnp.zeros(pool_a.shape[1:], pool_a.dtype)
    pool_b[rows] = jnp.zeros(pool_b.shape[1:], pool_b.dtype)
    pltpu.make_async_copy(sel_v, sel_v, sel_sem).wait()
    fill_slots(live_ref[0], sel_v[0], sel_v[1], table, layers, cap, rows)
    to_scalars = pltpu.make_async_copy(table, slots, table_sem)
    to_scalars.start()
    to_scalars.wait()
    load_wait(pool_a, pool_sem.at[0])

    def row_of(slot):
        return jnp.minimum(jnp.maximum(slots[slot, 0], 0), rows)

    def layer_peak(layer, carry):
        best = [jnp.zeros(pool.shape[1:], pool.dtype) for pool in (pool_a, pool_b)]
        for c in range(cap):
            row = row_of(layer * cap + c)
            best = [jnp.maximum(b, jnp.abs(pool[row])) for b, pool in zip(best, (pool_a, pool_b))]
        tops = [jnp.max(b.astype(f32), axis=0, keepdims=True) for b in best]
        top = jnp.maximum(tops[0], tops[1])
        for part in range(SLICES):
            pk_send[layer * SLICES + part] = top[:, part * half:(part + 1) * half]
        return carry

    def own_copy(src, dst, s_sem, r_sem, peer):
        return pltpu.make_async_remote_copy(
            src_ref=src, dst_ref=dst, send_sem=s_sem, recv_sem=r_sem,
            device_id={"own": peer}, device_id_type=pl.DeviceIdType.MESH)

    def rep_copy(src, dst, r_sem, peer):
        return pltpu.make_async_remote_copy(
            src_ref=src, dst_ref=dst, send_sem=small_send, recv_sem=r_sem,
            device_id={"rep": peer}, device_id_type=pl.DeviceIdType.MESH)

    def rep_share(table, r_sem):
        for k in range(1, rep_n):
            rep_copy(table.at[rep], table.at[rep], r_sem, lax.rem(rep + k, rep_n)).start()

    def arrived(dst, count, r_sem):
        own_copy(dst.at[pl.ds(0, count)], dst.at[pl.ds(0, count)], small_send, r_sem, lax.rem(me + 1, own_n)).wait_recv()

    eighth = loops // 8
    first, second = (0, eighth), (eighth, 2 * eighth)
    third, rest = (3 * eighth, 3 * eighth), (6 * eighth, loops - 6 * eighth)
    all_cols = (0, loops)

    def block_copy(peer, landing, cols, into, r_sem):
        lanes = pl.ds(cols[0] * period, cols[1] * period)
        return own_copy(send.at[peer, :, lanes], into.at[landing, :, lanes], send_sem, r_sem, peer)

    def flatten_layer(layer, cols):
        start, count = cols
        ranges = []
        for pool, begin in ((pool_a, 0), (pool_b, early)):
            t0, t1 = max(start * group, begin), min((start + count) * group, begin + pool.shape[1])
            if t0 < t1:
                ranges.append((pool, begin, t0, t1))
        for c in range(cap):
            row = row_of(layer * cap + c)
            for pool, begin, t0, t1 in ranges:
                block = pool[row, t0 - begin:t1 - begin, :].astype(f32)
                for q in range(tiles):
                    lo, hi = q * LANES, min(width, (q + 1) * LANES)
                    stage[q, c * tokens + t0:c * tokens + t1, 0:hi - lo] = block[:, lo:hi]

        def flatten(i, carry):
            rows_of = [
                jnp.concatenate(
                    [stage[q, pl.ds(i * group + j, cap, stride=tokens), :] for q in range(tiles)], axis=1)
                for j in range(group)
            ]
            for part in range(SLICES):
                joined = jnp.concatenate([r[:, part * half:(part + 1) * half] for r in rows_of], axis=1)
                at = pl.multiple_of(i * period, period)
                send[layer * SLICES + part, :, pl.ds(at, period)] = joined.astype(send.dtype)
            return carry

        lax.fori_loop(start, start + count, flatten, 0)

    def owner(layer, part):
        return layer * SLICES + lax.rem(my_slice + part, SLICES)

    across_first = list(range(1, SLICES)) + [0]
    order = [k for k in range(1, layers) if k != layers // 2]
    last = partner_layer(my_layer, layers, layers // 2)
    to_layer = [partner_layer(my_layer, layers, k) for k in order]
    from_layer = [partner_layer(my_layer, layers, layers - k) for k in order]
    mine_sem, last_sem = recv_sem.at[layers - 2], recv_sem.at[layers - 1]
    pk_sem, pr_sem, st_sem, pe_sem, er_sem = (small_recv.at[i] for i in range(5))

    def send_blocks(i, cols):
        for part in across_first:
            block_copy(owner(to_layer[i], part), me, cols, recv, recv_sem.at[i]).start()

    flatten_layer(to_layer[0], first)
    pl.semaphore_wait(barrier, own_n - 1 + rep_n - 1)
    send_blocks(0, first)
    load_wait(pool_b, pool_sem.at[1])
    lax.fori_loop(0, layers, layer_peak, 0, unroll=4)
    for k in range(1, own_n):
        peer = lax.rem(me + k, own_n)
        own_copy(pk_send.at[peer], pk_recv.at[me], small_send, pk_sem, peer).start()
    for cols in (second, third):
        flatten_layer(to_layer[0], cols)
        send_blocks(0, cols)
    flatten_layer(to_layer[0], rest)
    for i in range(1, layers - 2):
        flatten_layer(to_layer[i], all_cols)
    flatten_layer(last, all_cols)

    arrived(pk_recv, own_n - 1, pk_sem)
    best = pk_send[me]
    for k in range(1, own_n):
        best = jnp.maximum(best, pk_recv[lax.rem(me + k, own_n)])
    pk_rep[rep] = best
    rep_share(pk_rep, pr_sem)
    flatten_layer(my_layer, all_cols)
    arrived(pk_rep, rep_n - 1, pr_sem)
    for k in range(1, rep_n):
        best = jnp.maximum(best, pk_rep[lax.rem(rep + k, rep_n)])

    step = headroom * jnp.maximum(best, 1.0) / 127.0
    steps_ref[...] = step
    mine[...] = step
    for part in across_first:
        own_copy(mine, st_recv.at[me], small_send, st_sem, owner(last, part)).start()
    for i in range(1, layers - 2):
        send_blocks(i, all_cols)
    send_blocks(0, rest)
    for part in range(1, SLICES):
        block_copy(owner(my_layer, part), me, all_cols, recv, mine_sem).start()

    def wide(row):
        return jnp.broadcast_to(jnp.concatenate([row] * group, axis=1), (cap, period))

    def encode(source, target, src, one_step, total):
        step_wide = wide(one_step)
        inv_wide = wide(1.0 / one_step)

        def one(i, total):
            lanes = pl.ds(pl.multiple_of(i * period, period), period)
            x = source[src, :, lanes].astype(f32)
            y = jnp.clip(x * inv_wide, -127.0, 127.0).astype(codes_ref.dtype)
            target[src, :, lanes] = y
            diff = x - y.astype(f32) * step_wide
            return total + diff * diff
        return lax.fori_loop(0, loops, one, total)

    def fold(total):
        row = jnp.sum(total, axis=0, keepdims=True)
        folded = row[:, :half]
        for j in range(1, group):
            folded = folded + row[:, j * half:(j + 1) * half]
        return folded

    def blocks_arrived(count, r_sem):
        arrived(recv, count, r_sem)

    zero = jnp.zeros((cap, period), f32)
    codes_at = codes_ref.at[0, 0]
    total = encode(send, codes_at, me, step, zero)

    arrived(st_recv, SLICES, st_sem)
    for part in across_first:
        peer = owner(last, part)
        pe_send[peer] = fold(encode(send, send, peer, st_recv[peer], zero))
        own_copy(pe_send.at[peer], pe_recv.at[me], small_send, pe_sem, peer).start()
    for part in across_first:
        block_copy(owner(last, part), me, all_cols, codes_at, last_sem).start()

    blocks_arrived(SLICES, recv_sem.at[0])
    for part in across_first:
        total = encode(recv, codes_at, owner(from_layer[0], part), step, total)
    blocks_arrived(SLICES - 1, mine_sem)
    for part in range(1, SLICES):
        total = encode(recv, codes_at, owner(my_layer, part), step, total)
    for i in range(1, layers - 2):
        blocks_arrived(SLICES, recv_sem.at[i])
        for part in across_first:
            total = encode(recv, codes_at, owner(from_layer[i], part), step, total)

    error = fold(total)
    arrived(pe_recv, SLICES, pe_sem)
    for part in across_first:
        error = error + pe_recv[owner(last, part)]
    er_rep[rep] = error
    rep_share(er_rep, er_sem)
    arrived(er_rep, rep_n - 1, er_sem)
    whole = er_rep[0]
    for k in range(1, rep_n):
        whole = whole + er_rep[k]
    err_ref[...] = whole / (step * step * denominator)

    peer = lax.rem(me + 1, own_n)
    sent = own_n - 1 + 2 * (rep_n - 1) + 2 * SLICES
    many = pk_send.at[pl.ds(0, sent)]
    own_copy(many, many, small_send, last_sem, peer).wait_send()
    own_copy(send.at[pl.ds(0, own_n - 1)], recv.at[pl.ds(0, own_n - 1)], send_sem, last_sem, peer).wait_send()
    blocks_arrived(SLICES, last_sem)


def write_out(codes_v, steps_v, err_v, codes_ref, steps_ref, err_ref, sem, small_sem):
    own_n = codes_v.shape[2]
    for src in range(own_n):
        pltpu.make_async_copy(codes_v.at[0, 0, src], codes_ref.at[0, 0, src], sem).start()
    smalls = [pltpu.make_async_copy(steps_v, steps_ref, small_sem.at[0]),
              pltpu.make_async_copy(err_v, err_ref, small_sem.at[1])]
    for small in smalls:
        small.start()
    pltpu.make_async_copy(codes_v, codes_ref, sem).wait()
    for small in smalls:
        small.wait()


def body(block_pool, sel_index, sel_layer, counts):
    own_n = lax.axis_size("own")
    rep_n = lax.axis_size("rep")
    cap = sel_index.shape[0] // 4
    rows, tokens, width = block_pool.shape
    n_select = sel_index.shape[0]
    half = width // SLICES
    flat = tokens * half
    layers = own_n // SLICES
    f32, i32 = jnp.float32, jnp.int32
    dma = pltpu.SemaphoreType.DMA
    dtype = block_pool.dtype

    def row(n):
        return pltpu.VMEM((n, 1, half), f32)

    hbm = pl.BlockSpec(memory_space=pltpu.HBM)
    vmem = pl.BlockSpec(memory_space=pltpu.VMEM)
    codes, steps, err = pl.pallas_call(
        functools.partial(kernel, own_n, rep_n, cap),
        out_shape=(
            pltpu.VMEM((1, 1, own_n, cap, flat), dtype),
            pltpu.VMEM((1, half), f32),
            pltpu.VMEM((1, half), f32),
        ),
        in_specs=[pl.BlockSpec(memory_space=pltpu.SMEM)] + [hbm] * 3,
        out_specs=(vmem,) * 3,
        scratch_shapes=[
            pltpu.VMEM((2, 1, n_select), i32),
            pltpu.VMEM((layers * cap, LANES), i32),
            pltpu.SMEM((layers * cap, LANES), i32),
            pltpu.VMEM((rows + 1, tokens // 4, width), dtype),
            pltpu.VMEM((rows + 1, tokens - tokens // 4, width), dtype),
            pltpu.VMEM((pl.cdiv(width, LANES), cap * tokens, LANES), f32),
            pltpu.VMEM((own_n, cap, flat), dtype),
            pltpu.VMEM((own_n, cap, flat), dtype),
            row(own_n + 2 * rep_n + 2 * SLICES), row(own_n), row(rep_n),
            row(own_n), row(own_n), row(own_n), row(rep_n), pltpu.VMEM((1, half), f32),
            dma, dma, dma((2,)), dma, dma((layers,)), dma, dma((5,)),
        ],
        compiler_params=pltpu.CompilerParams(
            collective_id=0, has_side_effects=True, vmem_limit_bytes=(63 * 1024 * 1024 - own_n * cap * flat * 2)),
        name="latent_code",
    )(counts, sel_index[None], sel_layer[None], block_pool)
    return pl.pallas_call(
        write_out,
        out_shape=tuple(jax.ShapeDtypeStruct(x.shape, x.dtype) for x in (codes, steps, err)),
        in_specs=[vmem] * 3,
        out_specs=(hbm, hbm, hbm),
        scratch_shapes=[dma, dma((2,))],
        compiler_params=pltpu.CompilerParams(vmem_limit_bytes=4 * 1024 * 1024),
        name="write_out",
    )(codes, steps, err)


def solution(mesh):
    return jax.shard_map(
        body,
        mesh=mesh,
        in_specs=(
            P(("own", "rep"), None, None),
            P(("own", "rep")),
            P(("own", "rep")),
            P(("own", "rep")),
        ),
        out_specs=(P("own", "rep", None, None, None), P("own", None), P("own", None)),
        check_vma=False,
    )
```

```python
import functools
import math

import jax
import jax.numpy as jnp
from jax import lax
from jax.experimental import pallas as pl
from jax.experimental.pallas import tpu as pltpu
from jax.sharding import PartitionSpec as P

SLICES = 2
LANES = 128
PIECES = 8
headroom = 0.5


def ring_place(layer, layers):
    odd = layer % 2
    return odd * ((layer + 1) // 2) + (1 - odd) * lax.rem(layers - layer // 2, layers)


def ring_layer(place, layers):
    near = jnp.maximum(2 * place - 1, 0)
    return jnp.where(place <= layers // 2, near, 2 * (layers - place))


def partner_layer(my_layer, layers, k):
    return ring_layer(lax.rem(ring_place(my_layer, layers) + k, layers), layers)


def fill_slots(live, index_row, layer_row, table, layers, cap, empty):
    n_select = index_row.shape[1]
    is_live = lax.broadcasted_iota(jnp.int32, (1, n_select), 1) < live
    before = lax.broadcasted_iota(jnp.int32, (n_select, n_select), 0)
    after = lax.broadcasted_iota(jnp.int32, (n_select, n_select), 1)
    earlier = jnp.where(before < after, 1.0, 0.0)
    wanted = lax.broadcasted_iota(jnp.int32, (layers, n_select), 0)
    matches = jnp.where((layer_row == wanted) & is_live, 1.0, 0.0)
    ranking = jnp.dot(matches, earlier, preferred_element_type=jnp.float32)
    slot = lax.broadcasted_iota(jnp.int32, (cap, n_select), 0).astype(jnp.float32)
    shifted = index_row.astype(jnp.float32) - float(empty)
    for layer in range(layers):
        hit = (ranking[layer:layer + 1] == slot) & (matches[layer:layer + 1] > 0.5)
        found = jnp.sum(jnp.where(hit, shifted, 0.0), axis=1, keepdims=True) + float(empty)
        table[layer * cap:(layer + 1) * cap, :] = jnp.broadcast_to(found, (cap, LANES)).astype(jnp.int32)


def kernel(own_n, rep_n, cap, live_ref, index_hbm, layer_hbm, pool_ref, codes_ref, steps_ref, err_ref,
           sel_v, table, slots, pool_a, pool_b, stage, send, recv, pk_send, pk_recv, pk_rep,
           st_recv, pe_send, pe_recv, er_rep, mine,
           sel_sem, table_sem, pool_sem, send_sem, recv_sem, small_send, small_recv, late_sem):
    rows, tokens, width = pool_ref.shape
    half = width // SLICES
    group = LANES // math.gcd(half, LANES)
    period = group * half
    loops = tokens // group
    layers = own_n // SLICES
    me = lax.axis_index("own")
    rep = lax.axis_index("rep")
    my_layer = me // SLICES
    my_slice = me % SLICES
    tiles = stage.shape[0]
    denominator = float(own_n * rep_n * cap * tokens)
    f32 = jnp.float32
    early = pool_a.shape[1]

    sels = [pltpu.make_async_copy(index_hbm, sel_v.at[0], sel_sem),
            pltpu.make_async_copy(layer_hbm, sel_v.at[1], sel_sem)]
    for sel in sels:
        sel.start()
    barrier = pltpu.get_barrier_semaphore()
    is_inner = (my_layer > 0) & (my_layer < layers - 1)

    def greet(sem, axis, index):
        pl.semaphore_signal(sem, inc=1, device_id={axis: index}, device_id_type=pl.DeviceIdType.MESH)

    @pl.when(my_layer < layers - 1)
    def _():
        for k in range(1, own_n):
            greet(barrier, "own", lax.rem(me + k, own_n))

    @pl.when(my_layer == layers - 1)
    def _():
        for part in range(SLICES):
            greet(barrier, "own", part)
        for part in range(1, SLICES):
            greet(barrier, "own", my_layer * SLICES + lax.rem(my_slice + part, SLICES))
    for k in range(1, rep_n):
        greet(barrier, "rep", lax.rem(rep + k, rep_n))
    for pool, start, sem in ((pool_a, 0, pool_sem.at[0]), (pool_b, early, pool_sem.at[1])):
        for p in range(PIECES):
            here = pl.ds(p * (rows // PIECES), rows // PIECES)
            pltpu.make_async_copy(pool_ref.at[here, start:start + pool.shape[1]], pool.at[here], sem).start()

    def load_wait(pool, sem):
        pltpu.make_async_copy(pool_ref.at[:, 0:pool.shape[1]], pool.at[pl.ds(0, rows)], sem).wait()

    pool_a[rows] = jnp.zeros(pool_a.shape[1:], pool_a.dtype)
    pool_b[rows] = jnp.zeros(pool_b.shape[1:], pool_b.dtype)
    pltpu.make_async_copy(sel_v, sel_v, sel_sem).wait()
    fill_slots(live_ref[0], sel_v[0], sel_v[1], table, layers, cap, rows)
    to_scalars = pltpu.make_async_copy(table, slots, table_sem)
    to_scalars.start()
    to_scalars.wait()
    load_wait(pool_a, pool_sem.at[0])

    def row_of(slot):
        return jnp.minimum(jnp.maximum(slots[slot, 0], 0), rows)

    def layer_peak(layer, carry):
        best = [jnp.zeros(pool.shape[1:], pool.dtype) for pool in (pool_a, pool_b)]
        for c in range(cap):
            row = row_of(layer * cap + c)
            best = [jnp.maximum(b, jnp.abs(pool[row])) for b, pool in zip(best, (pool_a, pool_b))]
        tops = [jnp.max(b.astype(f32), axis=0, keepdims=True) for b in best]
        top = jnp.maximum(tops[0], tops[1])
        for part in range(SLICES):
            pk_send[layer * SLICES + part] = top[:, part * half:(part + 1) * half]
        return carry

    def own_copy(src, dst, s_sem, r_sem, peer):
        return pltpu.make_async_remote_copy(
            src_ref=src, dst_ref=dst, send_sem=s_sem, recv_sem=r_sem,
            device_id={"own": peer}, device_id_type=pl.DeviceIdType.MESH)

    def rep_copy(src, dst, r_sem, peer):
        return pltpu.make_async_remote_copy(
            src_ref=src, dst_ref=dst, send_sem=small_send, recv_sem=r_sem,
            device_id={"rep": peer}, device_id_type=pl.DeviceIdType.MESH)

    def rep_share(table, r_sem):
        for k in range(1, rep_n):
            rep_copy(table.at[rep], table.at[rep], r_sem, lax.rem(rep + k, rep_n)).start()

    def arrived(dst, count, r_sem):
        own_copy(dst.at[pl.ds(0, count)], dst.at[pl.ds(0, count)], small_send, r_sem, lax.rem(me + 1, own_n)).wait_recv()

    eighth = loops // 8
    raw = ((0, eighth), (eighth, eighth))
    coded = (2 * eighth, loops - 2 * eighth)
    early_cols = ((0, 3 * eighth), (3 * eighth, 3 * eighth))
    held = (6 * eighth, loops - 6 * eighth)
    all_cols = (0, loops)

    def block_copy(peer, landing, cols, into, r_sem):
        lanes = pl.ds(cols[0] * period, cols[1] * period)
        return own_copy(send.at[peer, :, lanes], into.at[landing, :, lanes], send_sem, r_sem, peer)

    def flatten_layer(layer, cols):
        start, count = cols
        ranges = []
        for pool, begin in ((pool_a, 0), (pool_b, early)):
            t0, t1 = max(start * group, begin), min((start + count) * group, begin + pool.shape[1])
            if t0 < t1:
                ranges.append((pool, begin, t0, t1))
        for c in range(cap):
            row = row_of(layer * cap + c)
            for pool, begin, t0, t1 in ranges:
                block = pool[row, t0 - begin:t1 - begin, :].astype(f32)
                for q in range(tiles):
                    lo, hi = q * LANES, min(width, (q + 1) * LANES)
                    stage[q, c * tokens + t0:c * tokens + t1, 0:hi - lo] = block[:, lo:hi]

        def flatten(i, carry):
            rows_of = [
                jnp.concatenate(
                    [stage[q, pl.ds(i * group + j, cap, stride=tokens), :] for q in range(tiles)], axis=1)
                for j in range(group)
            ]
            for part in range(SLICES):
                joined = jnp.concatenate([r[:, part * half:(part + 1) * half] for r in rows_of], axis=1)
                at = pl.multiple_of(i * period, period)
                send[layer * SLICES + part, :, pl.ds(at, period)] = joined.astype(send.dtype)
            return carry

        lax.fori_loop(start, start + count, flatten, 0)

    def owner(layer, part):
        return layer * SLICES + lax.rem(my_slice + part, SLICES)

    across_first = list(range(1, SLICES)) + [0]
    order = [k for k in range(1, layers) if k != layers // 2]
    last = partner_layer(my_layer, layers, layers // 2)
    to_layer = [partner_layer(my_layer, layers, k) for k in order]
    from_layer = [partner_layer(my_layer, layers, layers - k) for k in order]
    mine_sem, last_sem, raw_sem = (recv_sem.at[layers - 2 + i] for i in range(3))
    pk_sem, pr_sem, st_sem, pe_sem, er_sem = (small_recv.at[i] for i in range(5))

    def send_blocks(i, cols):
        for part in across_first:
            block_copy(owner(to_layer[i], part), me, cols, recv, recv_sem.at[i]).start()

    def send_last(cols, into, r_sem):
        for part in across_first:
            block_copy(owner(last, part), me, cols, into, r_sem).start()

    flatten_layer(last, raw[0])
    pl.semaphore_wait(barrier, own_n - 1 + rep_n - 1 - jnp.where(is_inner, SLICES, 0))
    send_last(raw[0], recv, raw_sem)

    @pl.when(my_layer == 0)
    def _():
        for layer in range(1, layers - 1):
            greet(late_sem, "own", layer * SLICES + my_slice)

    flatten_layer(last, raw[1])
    send_last(raw[1], recv, raw_sem)
    load_wait(pool_b, pool_sem.at[1])
    lax.fori_loop(0, layers, layer_peak, 0, unroll=4)
    flatten_layer(to_layer[0], early_cols[0])

    @pl.when(is_inner)
    def _():
        pl.semaphore_wait(late_sem, 1)

    for k in range(1, own_n):
        peer = lax.rem(me + k, own_n)
        own_copy(pk_send.at[peer], pk_recv.at[me], small_send, pk_sem, peer).start()
    send_blocks(0, early_cols[0])
    flatten_layer(to_layer[0], early_cols[1])
    send_blocks(0, early_cols[1])
    flatten_layer(to_layer[0], held)
    for i in range(1, layers - 2):
        flatten_layer(to_layer[i], all_cols)
    flatten_layer(last, coded)

    arrived(pk_recv, own_n - 1, pk_sem)
    best = pk_send[me]
    for k in range(1, own_n):
        best = jnp.maximum(best, pk_recv[lax.rem(me + k, own_n)])
    pk_rep[rep] = best
    rep_share(pk_rep, pr_sem)
    flatten_layer(my_layer, all_cols)
    arrived(pk_rep, rep_n - 1, pr_sem)
    for k in range(1, rep_n):
        best = jnp.maximum(best, pk_rep[lax.rem(rep + k, rep_n)])

    step = headroom * jnp.maximum(best, 1.0) / 127.0
    steps_ref[...] = step
    mine[...] = step
    for part in across_first:
        own_copy(mine, st_recv.at[me], small_send, st_sem, owner(last, part)).start()
    for i in range(1, layers - 2):
        send_blocks(i, all_cols)
    send_blocks(0, held)
    for part in range(1, SLICES):
        block_copy(owner(my_layer, part), me, all_cols, recv, mine_sem).start()

    def wide(row):
        return jnp.broadcast_to(jnp.concatenate([row] * group, axis=1), (cap, period))

    def encode(source, target, src, one_step, total, cols=all_cols):
        step_wide = wide(one_step)
        inv_wide = wide(1.0 / one_step)

        def one(i, total):
            lanes = pl.ds(pl.multiple_of(i * period, period), period)
            x = source[src, :, lanes].astype(f32)
            y = jnp.clip(x * inv_wide, -127.0, 127.0).astype(codes_ref.dtype)
            target[src, :, lanes] = y
            diff = x - y.astype(f32) * step_wide
            return total + diff * diff
        return lax.fori_loop(cols[0], cols[0] + cols[1], one, total)

    def fold(total):
        row = jnp.sum(total, axis=0, keepdims=True)
        folded = row[:, :half]
        for j in range(1, group):
            folded = folded + row[:, j * half:(j + 1) * half]
        return folded

    def blocks_arrived(count, r_sem, n_loops=loops):
        some = recv.at[pl.ds(0, count), :, pl.ds(0, n_loops * period)]
        own_copy(some, some, small_send, r_sem, lax.rem(me + 1, own_n)).wait_recv()

    zero = jnp.zeros((cap, period), f32)
    codes_at = codes_ref.at[0, 0]
    total = encode(send, codes_at, me, step, zero)

    arrived(st_recv, SLICES, st_sem)
    for part in across_first:
        peer = owner(last, part)
        pe_send[peer] = fold(encode(send, send, peer, st_recv[peer], zero, coded))
        own_copy(pe_send.at[peer], pe_recv.at[me], small_send, pe_sem, peer).start()
    send_last(coded, codes_at, last_sem)

    blocks_arrived(SLICES, raw_sem, coded[0])
    for part in across_first:
        total = encode(recv, codes_at, owner(last, part), step, total, (0, coded[0]))
    blocks_arrived(SLICES, recv_sem.at[0])
    for part in across_first:
        total = encode(recv, codes_at, owner(from_layer[0], part), step, total)
    blocks_arrived(SLICES - 1, mine_sem)
    for part in range(1, SLICES):
        total = encode(recv, codes_at, owner(my_layer, part), step, total)
    for i in range(1, layers - 2):
        blocks_arrived(SLICES, recv_sem.at[i])
        for part in across_first:
            total = encode(recv, codes_at, owner(from_layer[i], part), step, total)

    error = fold(total)
    arrived(pe_recv, SLICES, pe_sem)
    for part in across_first:
        error = error + pe_recv[owner(last, part)]
    er_rep[rep] = error
    rep_share(er_rep, er_sem)
    arrived(er_rep, rep_n - 1, er_sem)
    whole = er_rep[0]
    for k in range(1, rep_n):
        whole = whole + er_rep[k]
    err_ref[...] = whole / (step * step * denominator)

    peer = lax.rem(me + 1, own_n)
    sent = own_n - 1 + 2 * (rep_n - 1) + 2 * SLICES
    many = pk_send.at[pl.ds(0, sent)]
    own_copy(many, many, small_send, last_sem, peer).wait_send()
    own_copy(send.at[pl.ds(0, own_n - 1)], recv.at[pl.ds(0, own_n - 1)], send_sem, last_sem, peer).wait_send()
    blocks_arrived(SLICES, last_sem, coded[1])


def write_out(codes_v, steps_v, err_v, codes_ref, steps_ref, err_ref, sem, small_sem):
    own_n = codes_v.shape[2]
    for src in range(own_n):
        pltpu.make_async_copy(codes_v.at[0, 0, src], codes_ref.at[0, 0, src], sem).start()
    smalls = [pltpu.make_async_copy(steps_v, steps_ref, small_sem.at[0]),
              pltpu.make_async_copy(err_v, err_ref, small_sem.at[1])]
    for small in smalls:
        small.start()
    pltpu.make_async_copy(codes_v, codes_ref, sem).wait()
    for small in smalls:
        small.wait()


def body(block_pool, sel_index, sel_layer, counts):
    own_n = lax.axis_size("own")
    rep_n = lax.axis_size("rep")
    cap = sel_index.shape[0] // 4
    rows, tokens, width = block_pool.shape
    n_select = sel_index.shape[0]
    half = width // SLICES
    flat = tokens * half
    layers = own_n // SLICES
    f32, i32 = jnp.float32, jnp.int32
    dma = pltpu.SemaphoreType.DMA
    dtype = block_pool.dtype

    def row(n):
        return pltpu.VMEM((n, 1, half), f32)

    hbm = pl.BlockSpec(memory_space=pltpu.HBM)
    vmem = pl.BlockSpec(memory_space=pltpu.VMEM)
    codes, steps, err = pl.pallas_call(
        functools.partial(kernel, own_n, rep_n, cap),
        out_shape=(
            pltpu.VMEM((1, 1, own_n, cap, flat), dtype),
            pltpu.VMEM((1, half), f32),
            pltpu.VMEM((1, half), f32),
        ),
        in_specs=[pl.BlockSpec(memory_space=pltpu.SMEM)] + [hbm] * 3,
        out_specs=(vmem,) * 3,
        scratch_shapes=[
            pltpu.VMEM((2, 1, n_select), i32),
            pltpu.VMEM((layers * cap, LANES), i32),
            pltpu.SMEM((layers * cap, LANES), i32),
            pltpu.VMEM((rows + 1, tokens // 4, width), dtype),
            pltpu.VMEM((rows + 1, tokens - tokens // 4, width), dtype),
            pltpu.VMEM((pl.cdiv(width, LANES), cap * tokens, LANES), f32),
            pltpu.VMEM((own_n, cap, flat), dtype),
            pltpu.VMEM((own_n, cap, flat), dtype),
            row(own_n + 2 * rep_n + 2 * SLICES), row(own_n), row(rep_n),
            row(own_n), row(own_n), row(own_n), row(rep_n), pltpu.VMEM((1, half), f32),
            dma, dma, dma((2,)), dma, dma((layers + 1,)), dma, dma((5,)), pltpu.SemaphoreType.REGULAR,
        ],
        compiler_params=pltpu.CompilerParams(
            collective_id=0, has_side_effects=True, vmem_limit_bytes=(63 * 1024 * 1024 - own_n * cap * flat * 2)),
        name="latent_code",
    )(counts, sel_index[None], sel_layer[None], block_pool)
    return pl.pallas_call(
        write_out,
        out_shape=tuple(jax.ShapeDtypeStruct(x.shape, x.dtype) for x in (codes, steps, err)),
        in_specs=[vmem] * 3,
        out_specs=(hbm, hbm, hbm),
        scratch_shapes=[dma, dma((2,))],
        compiler_params=pltpu.CompilerParams(vmem_limit_bytes=4 * 1024 * 1024),
        name="write_out",
    )(codes, steps, err)


def solution(mesh):
    return jax.shard_map(
        body,
        mesh=mesh,
        in_specs=(
            P(("own", "rep"), None, None),
            P(("own", "rep")),
            P(("own", "rep")),
            P(("own", "rep")),
        ),
        out_specs=(P("own", "rep", None, None, None), P("own", None), P("own", None)),
        check_vma=False,
    )
```

```python
import functools
import math

import jax
import jax.numpy as jnp
from jax import lax
from jax.experimental import pallas as pl
from jax.experimental.pallas import tpu as pltpu
from jax.sharding import PartitionSpec as P

SLICES = 2
LANES = 128
PIECES = 8
headroom = 0.5


def ring_place(layer, layers):
    odd = layer % 2
    return odd * ((layer + 1) // 2) + (1 - odd) * lax.rem(layers - layer // 2, layers)


def ring_layer(place, layers):
    near = jnp.maximum(2 * place - 1, 0)
    return jnp.where(place <= layers // 2, near, 2 * (layers - place))


def partner_layer(my_layer, layers, k):
    return ring_layer(lax.rem(ring_place(my_layer, layers) + k, layers), layers)


def fill_slots(live, index_row, layer_row, table, layers, cap, empty):
    n_select = index_row.shape[1]
    is_live = lax.broadcasted_iota(jnp.int32, (1, n_select), 1) < live
    before = lax.broadcasted_iota(jnp.int32, (n_select, n_select), 0)
    after = lax.broadcasted_iota(jnp.int32, (n_select, n_select), 1)
    earlier = jnp.where(before < after, 1.0, 0.0)
    wanted = lax.broadcasted_iota(jnp.int32, (layers, n_select), 0)
    matches = jnp.where((layer_row == wanted) & is_live, 1.0, 0.0)
    ranking = jnp.dot(matches, earlier, preferred_element_type=jnp.float32)
    slot = lax.broadcasted_iota(jnp.int32, (cap, n_select), 0).astype(jnp.float32)
    shifted = index_row.astype(jnp.float32) - float(empty)
    place = lax.broadcasted_iota(jnp.int32, (cap, table.shape[1]), 1)
    spread = jnp.zeros((cap, table.shape[1]), jnp.float32)
    for layer in range(layers):
        hit = (ranking[layer:layer + 1] == slot) & (matches[layer:layer + 1] > 0.5)
        found = jnp.sum(jnp.where(hit, shifted, 0.0), axis=1, keepdims=True) + float(empty)
        here = place == layer * cap + lax.broadcasted_iota(jnp.int32, place.shape, 0)
        spread = spread + jnp.where(here, found, 0.0)
    row = jnp.sum(spread, axis=0, keepdims=True)
    table[...] = row.astype(jnp.int32)
    return row


def kernel(own_n, rep_n, cap, live_ref, index_hbm, layer_hbm, pool_ref, codes_ref, steps_ref, err_ref,
           sel_v, table, slots, pool_a, pool_b, stage, send, recv, pk_send, pk_recv, pk_rep,
           st_recv, pe_send, pe_recv, er_rep, mine,
           sel_sem, table_sem, pool_sem, send_sem, recv_sem, small_send, small_recv, late_sem):
    rows, tokens, width = pool_ref.shape
    half = width // SLICES
    group = LANES // math.gcd(half, LANES)
    period = group * half
    loops = tokens // group
    layers = own_n // SLICES
    me = lax.axis_index("own")
    rep = lax.axis_index("rep")
    my_layer = me // SLICES
    my_slice = me % SLICES
    tiles = stage.shape[0]
    denominator = float(own_n * rep_n * cap * tokens)
    f32 = jnp.float32
    early = pool_a.shape[1]

    sels = [pltpu.make_async_copy(index_hbm, sel_v.at[0], sel_sem),
            pltpu.make_async_copy(layer_hbm, sel_v.at[1], sel_sem)]
    for sel in sels:
        sel.start()
    barrier = pltpu.get_barrier_semaphore()
    is_inner = (my_layer > 0) & (my_layer < layers - 1)

    def greet(sem, axis, index):
        pl.semaphore_signal(sem, inc=1, device_id={axis: index}, device_id_type=pl.DeviceIdType.MESH)

    @pl.when(my_layer < layers - 1)
    def _():
        for k in range(1, own_n):
            greet(barrier, "own", lax.rem(me + k, own_n))

    @pl.when(my_layer == layers - 1)
    def _():
        for part in range(SLICES):
            greet(barrier, "own", part)
        for part in range(1, SLICES):
            greet(barrier, "own", my_layer * SLICES + lax.rem(my_slice + part, SLICES))
    for k in range(1, rep_n):
        greet(barrier, "rep", lax.rem(rep + k, rep_n))
    for pool, start, sem in ((pool_a, 0, pool_sem.at[0]), (pool_b, early, pool_sem.at[1])):
        for p in range(PIECES):
            here = pl.ds(p * (rows // PIECES), rows // PIECES)
            pltpu.make_async_copy(pool_ref.at[here, start:start + pool.shape[1]], pool.at[here], sem).start()

    def load_wait(pool, sem):
        pltpu.make_async_copy(pool_ref.at[:, 0:pool.shape[1]], pool.at[pl.ds(0, rows)], sem).wait()

    pool_a[rows] = jnp.zeros(pool_a.shape[1:], pool_a.dtype)
    pool_b[rows] = jnp.zeros(pool_b.shape[1:], pool_b.dtype)
    pltpu.make_async_copy(sel_v, sel_v, sel_sem).wait()
    filled = fill_slots(live_ref[0], sel_v[0], sel_v[1], table, layers, cap, rows)
    to_scalars = pltpu.make_async_copy(table, slots, table_sem)
    to_scalars.start()
    last = partner_layer(my_layer, layers, layers // 2)
    place = lax.broadcasted_iota(jnp.int32, filled.shape, 1)
    first_rows = []
    for c in range(cap):
        row = jnp.sum(jnp.where(place == last * cap + c, filled, 0.0)).astype(jnp.int32)
        first_rows.append(jnp.minimum(jnp.maximum(row, 0), rows))
    load_wait(pool_a, pool_sem.at[0])

    def row_of(slot):
        return jnp.minimum(jnp.maximum(slots[0, slot], 0), rows)

    def layer_peak(layer, carry):
        best = [jnp.zeros(pool.shape[1:], pool.dtype) for pool in (pool_a, pool_b)]
        for c in range(cap):
            row = row_of(layer * cap + c)
            best = [jnp.maximum(b, jnp.abs(pool[row])) for b, pool in zip(best, (pool_a, pool_b))]
        tops = [jnp.max(b.astype(f32), axis=0, keepdims=True) for b in best]
        top = jnp.maximum(tops[0], tops[1])
        for part in range(SLICES):
            pk_send[layer * SLICES + part] = top[:, part * half:(part + 1) * half]
        return carry

    def own_copy(src, dst, s_sem, r_sem, peer):
        return pltpu.make_async_remote_copy(
            src_ref=src, dst_ref=dst, send_sem=s_sem, recv_sem=r_sem,
            device_id={"own": peer}, device_id_type=pl.DeviceIdType.MESH)

    def rep_copy(src, dst, r_sem, peer):
        return pltpu.make_async_remote_copy(
            src_ref=src, dst_ref=dst, send_sem=small_send, recv_sem=r_sem,
            device_id={"rep": peer}, device_id_type=pl.DeviceIdType.MESH)

    def rep_share(table, r_sem):
        for k in range(1, rep_n):
            rep_copy(table.at[rep], table.at[rep], r_sem, lax.rem(rep + k, rep_n)).start()

    def arrived(dst, count, r_sem):
        own_copy(dst.at[pl.ds(0, count)], dst.at[pl.ds(0, count)], small_send, r_sem, lax.rem(me + 1, own_n)).wait_recv()

    eighth = loops // 8
    raw = ((0, eighth), (eighth, eighth))
    coded = (2 * eighth, loops - 2 * eighth)
    early_cols = ((0, eighth), (eighth, 5 * eighth))
    held = (6 * eighth, loops - 6 * eighth)
    all_cols = (0, loops)

    def block_copy(peer, landing, cols, into, r_sem):
        lanes = pl.ds(cols[0] * period, cols[1] * period)
        return own_copy(send.at[peer, :, lanes], into.at[landing, :, lanes], send_sem, r_sem, peer)

    def flatten_layer(layer, cols, known=None):
        start, count = cols
        ranges = []
        for pool, begin in ((pool_a, 0), (pool_b, early)):
            t0, t1 = max(start * group, begin), min((start + count) * group, begin + pool.shape[1])
            if t0 < t1:
                ranges.append((pool, begin, t0, t1))
        for c in range(cap):
            row = known[c] if known else row_of(layer * cap + c)
            for pool, begin, t0, t1 in ranges:
                block = pool[row, t0 - begin:t1 - begin, :].astype(f32)
                for q in range(tiles):
                    lo, hi = q * LANES, min(width, (q + 1) * LANES)
                    stage[q, c * tokens + t0:c * tokens + t1, 0:hi - lo] = block[:, lo:hi]

        def flatten(i, carry):
            rows_of = [
                jnp.concatenate(
                    [stage[q, pl.ds(i * group + j, cap, stride=tokens), :] for q in range(tiles)], axis=1)
                for j in range(group)
            ]
            for part in range(SLICES):
                joined = jnp.concatenate([r[:, part * half:(part + 1) * half] for r in rows_of], axis=1)
                at = pl.multiple_of(i * period, period)
                send[layer * SLICES + part, :, pl.ds(at, period)] = joined.astype(send.dtype)
            return carry

        lax.fori_loop(start, start + count, flatten, 0)

    def owner(layer, part):
        return layer * SLICES + lax.rem(my_slice + part, SLICES)

    across_first = list(range(1, SLICES)) + [0]
    order = [k for k in range(1, layers) if k != layers // 2]
    to_layer = [partner_layer(my_layer, layers, k) for k in order]
    from_layer = [partner_layer(my_layer, layers, layers - k) for k in order]
    mine_sem, last_sem, raw_sem = (recv_sem.at[layers - 2 + i] for i in range(3))
    pk_sem, pr_sem, st_sem, pe_sem, er_sem = (small_recv.at[i] for i in range(5))

    def send_blocks(i, cols):
        for part in across_first:
            block_copy(owner(to_layer[i], part), me, cols, recv, recv_sem.at[i]).start()

    def send_last(cols, into, r_sem):
        for part in across_first:
            block_copy(owner(last, part), me, cols, into, r_sem).start()

    flatten_layer(last, raw[0], first_rows)
    pl.semaphore_wait(barrier, own_n - 1 + rep_n - 1 - jnp.where(is_inner, SLICES, 0))
    send_last(raw[0], recv, raw_sem)

    @pl.when(my_layer == 0)
    def _():
        for layer in range(1, layers - 1):
            greet(late_sem, "own", layer * SLICES + my_slice)

    to_scalars.wait()
    flatten_layer(last, raw[1])
    send_last(raw[1], recv, raw_sem)
    load_wait(pool_b, pool_sem.at[1])
    lax.fori_loop(0, layers, layer_peak, 0, unroll=4)
    flatten_layer(to_layer[0], early_cols[0])
    is_later = is_inner & (to_layer[0] == layers - 1)

    @pl.when(jnp.logical_not(is_later))
    def _():
        send_blocks(0, early_cols[0])

    flatten_layer(to_layer[0], early_cols[1])

    @pl.when(is_inner)
    def _():
        pl.semaphore_wait(late_sem, 1)

    for k in range(1, own_n):
        peer = lax.rem(me + k, own_n)
        own_copy(pk_send.at[peer], pk_recv.at[me], small_send, pk_sem, peer).start()

    @pl.when(is_later)
    def _():
        send_blocks(0, early_cols[0])

    send_blocks(0, early_cols[1])
    flatten_layer(to_layer[0], held)
    for i in range(1, layers - 2):
        flatten_layer(to_layer[i], all_cols)
    flatten_layer(last, coded)

    arrived(pk_recv, own_n - 1, pk_sem)
    best = pk_send[me]
    for k in range(1, own_n):
        best = jnp.maximum(best, pk_recv[lax.rem(me + k, own_n)])
    pk_rep[rep] = best
    rep_share(pk_rep, pr_sem)
    flatten_layer(my_layer, all_cols)
    arrived(pk_rep, rep_n - 1, pr_sem)
    for k in range(1, rep_n):
        best = jnp.maximum(best, pk_rep[lax.rem(rep + k, rep_n)])

    step = headroom * jnp.maximum(best, 1.0) / 127.0
    steps_ref[...] = step
    mine[...] = step
    for part in across_first:
        own_copy(mine, st_recv.at[me], small_send, st_sem, owner(last, part)).start()
    for i in range(1, layers - 2):
        send_blocks(i, all_cols)
    send_blocks(0, held)
    for part in range(1, SLICES):
        block_copy(owner(my_layer, part), me, all_cols, recv, mine_sem).start()

    def wide(row):
        return jnp.broadcast_to(jnp.concatenate([row] * group, axis=1), (cap, period))

    def encode(source, target, src, one_step, total, cols=all_cols):
        step_wide = wide(one_step)
        inv_wide = wide(1.0 / one_step)

        def one(i, total):
            lanes = pl.ds(pl.multiple_of(i * period, period), period)
            x = source[src, :, lanes].astype(f32)
            y = jnp.clip(x * inv_wide, -127.0, 127.0).astype(codes_ref.dtype)
            target[src, :, lanes] = y
            diff = x - y.astype(f32) * step_wide
            return total + diff * diff
        return lax.fori_loop(cols[0], cols[0] + cols[1], one, total)

    def fold(total):
        row = jnp.sum(total, axis=0, keepdims=True)
        folded = row[:, :half]
        for j in range(1, group):
            folded = folded + row[:, j * half:(j + 1) * half]
        return folded

    def blocks_arrived(count, r_sem, n_loops=loops):
        some = recv.at[pl.ds(0, count), :, pl.ds(0, n_loops * period)]
        own_copy(some, some, small_send, r_sem, lax.rem(me + 1, own_n)).wait_recv()

    zero = jnp.zeros((cap, period), f32)
    codes_at = codes_ref.at[0, 0]
    total = encode(send, codes_at, me, step, zero)

    arrived(st_recv, SLICES, st_sem)
    for part in across_first:
        peer = owner(last, part)
        pe_send[peer] = fold(encode(send, send, peer, st_recv[peer], zero, coded))
        own_copy(pe_send.at[peer], pe_recv.at[me], small_send, pe_sem, peer).start()
    send_last(coded, codes_at, last_sem)

    blocks_arrived(SLICES, raw_sem, coded[0])
    for part in across_first:
        total = encode(recv, codes_at, owner(last, part), step, total, (0, coded[0]))
    blocks_arrived(SLICES, recv_sem.at[0])
    for part in across_first:
        total = encode(recv, codes_at, owner(from_layer[0], part), step, total)
    blocks_arrived(SLICES - 1, mine_sem)
    for part in range(1, SLICES):
        total = encode(recv, codes_at, owner(my_layer, part), step, total)
    for i in range(1, layers - 2):
        blocks_arrived(SLICES, recv_sem.at[i])
        for part in across_first:
            total = encode(recv, codes_at, owner(from_layer[i], part), step, total)

    error = fold(total)
    arrived(pe_recv, SLICES, pe_sem)
    for part in across_first:
        error = error + pe_recv[owner(last, part)]
    er_rep[rep] = error
    rep_share(er_rep, er_sem)
    arrived(er_rep, rep_n - 1, er_sem)
    whole = er_rep[0]
    for k in range(1, rep_n):
        whole = whole + er_rep[k]
    err_ref[...] = whole / (step * step * denominator)

    peer = lax.rem(me + 1, own_n)
    sent = own_n - 1 + 2 * (rep_n - 1) + 2 * SLICES
    many = pk_send.at[pl.ds(0, sent)]
    own_copy(many, many, small_send, last_sem, peer).wait_send()
    own_copy(send.at[pl.ds(0, own_n - 1)], recv.at[pl.ds(0, own_n - 1)], send_sem, last_sem, peer).wait_send()
    blocks_arrived(SLICES, last_sem, coded[1])


def write_out(codes_v, steps_v, err_v, codes_ref, steps_ref, err_ref, sem, small_sem):
    own_n = codes_v.shape[2]
    for src in range(own_n):
        pltpu.make_async_copy(codes_v.at[0, 0, src], codes_ref.at[0, 0, src], sem).start()
    smalls = [pltpu.make_async_copy(steps_v, steps_ref, small_sem.at[0]),
              pltpu.make_async_copy(err_v, err_ref, small_sem.at[1])]
    for small in smalls:
        small.start()
    pltpu.make_async_copy(codes_v, codes_ref, sem).wait()
    for small in smalls:
        small.wait()


def body(block_pool, sel_index, sel_layer, counts):
    own_n = lax.axis_size("own")
    rep_n = lax.axis_size("rep")
    cap = sel_index.shape[0] // 4
    rows, tokens, width = block_pool.shape
    n_select = sel_index.shape[0]
    half = width // SLICES
    flat = tokens * half
    layers = own_n // SLICES
    f32, i32 = jnp.float32, jnp.int32
    dma = pltpu.SemaphoreType.DMA
    dtype = block_pool.dtype

    def row(n):
        return pltpu.VMEM((n, 1, half), f32)

    hbm = pl.BlockSpec(memory_space=pltpu.HBM)
    vmem = pl.BlockSpec(memory_space=pltpu.VMEM)
    codes, steps, err = pl.pallas_call(
        functools.partial(kernel, own_n, rep_n, cap),
        out_shape=(
            pltpu.VMEM((1, 1, own_n, cap, flat), dtype),
            pltpu.VMEM((1, half), f32),
            pltpu.VMEM((1, half), f32),
        ),
        in_specs=[pl.BlockSpec(memory_space=pltpu.SMEM)] + [hbm] * 3,
        out_specs=(vmem,) * 3,
        scratch_shapes=[
            pltpu.VMEM((2, 1, n_select), i32),
            pltpu.VMEM((1, pl.cdiv(layers * cap, LANES) * LANES), i32),
            pltpu.SMEM((1, pl.cdiv(layers * cap, LANES) * LANES), i32),
            pltpu.VMEM((rows + 1, tokens // 4, width), dtype),
            pltpu.VMEM((rows + 1, tokens - tokens // 4, width), dtype),
            pltpu.VMEM((pl.cdiv(width, LANES), cap * tokens, LANES), f32),
            pltpu.VMEM((own_n, cap, flat), dtype),
            pltpu.VMEM((own_n, cap, flat), dtype),
            row(own_n + 2 * rep_n + 2 * SLICES), row(own_n), row(rep_n),
            row(own_n), row(own_n), row(own_n), row(rep_n), pltpu.VMEM((1, half), f32),
            dma, dma, dma((2,)), dma, dma((layers + 1,)), dma, dma((5,)), pltpu.SemaphoreType.REGULAR,
        ],
        compiler_params=pltpu.CompilerParams(
            collective_id=0, has_side_effects=True, vmem_limit_bytes=(63 * 1024 * 1024 - own_n * cap * flat * 2)),
        name="latent_code",
    )(counts, sel_index[None], sel_layer[None], block_pool)
    return pl.pallas_call(
        write_out,
        out_shape=tuple(jax.ShapeDtypeStruct(x.shape, x.dtype) for x in (codes, steps, err)),
        in_specs=[vmem] * 3,
        out_specs=(hbm, hbm, hbm),
        scratch_shapes=[dma, dma((2,))],
        compiler_params=pltpu.CompilerParams(vmem_limit_bytes=4 * 1024 * 1024),
        name="write_out",
    )(codes, steps, err)


def solution(mesh):
    return jax.shard_map(
        body,
        mesh=mesh,
        in_specs=(
            P(("own", "rep"), None, None),
            P(("own", "rep")),
            P(("own", "rep")),
            P(("own", "rep")),
        ),
        out_specs=(P("own", "rep", None, None, None), P("own", None), P("own", None)),
        check_vma=False,
    )
```

```python
import functools
import math

import jax
import jax.numpy as jnp
from jax import lax
from jax.experimental import pallas as pl
from jax.experimental.pallas import tpu as pltpu
from jax.sharding import PartitionSpec as P

SLICES = 2
LANES = 128
PIECES = 8
headroom = 0.5


def ring_place(layer, layers):
    odd = layer % 2
    return odd * ((layer + 1) // 2) + (1 - odd) * lax.rem(layers - layer // 2, layers)


def ring_layer(place, layers):
    near = jnp.maximum(2 * place - 1, 0)
    return jnp.where(place <= layers // 2, near, 2 * (layers - place))


def partner_layer(my_layer, layers, k):
    return ring_layer(lax.rem(ring_place(my_layer, layers) + k, layers), layers)


def fill_slots(live, index_row, layer_row, table, layers, cap, empty):
    n_select = index_row.shape[1]
    is_live = lax.broadcasted_iota(jnp.int32, (1, n_select), 1) < live
    before = lax.broadcasted_iota(jnp.int32, (n_select, n_select), 0)
    after = lax.broadcasted_iota(jnp.int32, (n_select, n_select), 1)
    earlier = jnp.where(before < after, 1.0, 0.0)
    wanted = lax.broadcasted_iota(jnp.int32, (layers, n_select), 0)
    matches = jnp.where((layer_row == wanted) & is_live, 1.0, 0.0)
    ranking = jnp.dot(matches, earlier, preferred_element_type=jnp.float32)
    slot = lax.broadcasted_iota(jnp.int32, (cap, n_select), 0).astype(jnp.float32)
    shifted = index_row.astype(jnp.float32) - float(empty)
    place = lax.broadcasted_iota(jnp.int32, (cap, table.shape[1]), 1)
    spread = jnp.zeros((cap, table.shape[1]), jnp.float32)
    for layer in range(layers):
        hit = (ranking[layer:layer + 1] == slot) & (matches[layer:layer + 1] > 0.5)
        found = jnp.sum(jnp.where(hit, shifted, 0.0), axis=1, keepdims=True) + float(empty)
        here = place == layer * cap + lax.broadcasted_iota(jnp.int32, place.shape, 0)
        spread = spread + jnp.where(here, found, 0.0)
    row = jnp.sum(spread, axis=0, keepdims=True)
    table[...] = row.astype(jnp.int32)
    return row


def kernel(own_n, rep_n, cap, live_ref, index_hbm, layer_hbm, pool_ref, codes_ref, steps_ref, err_ref,
           sel_v, table, slots, pool_a, pool_b, stage, send, recv, pk_send, pk_recv, pk_rep,
           st_recv, pe_send, pe_recv, er_rep, mine,
           sel_sem, table_sem, pool_sem, send_sem, recv_sem, small_send, small_recv, late_sem):
    rows, tokens, width = pool_ref.shape
    half = width // SLICES
    group = LANES // math.gcd(half, LANES)
    period = group * half
    loops = tokens // group
    layers = own_n // SLICES
    me = lax.axis_index("own")
    rep = lax.axis_index("rep")
    my_layer = me // SLICES
    my_slice = me % SLICES
    tiles = stage.shape[0]
    denominator = float(own_n * rep_n * cap * tokens)
    f32 = jnp.float32
    early = pool_a.shape[1]

    sels = [pltpu.make_async_copy(index_hbm, sel_v.at[0], sel_sem),
            pltpu.make_async_copy(layer_hbm, sel_v.at[1], sel_sem)]
    for sel in sels:
        sel.start()
    barrier = pltpu.get_barrier_semaphore()
    is_inner = (my_layer > 0) & (my_layer < layers - 1)

    def greet(sem, axis, index):
        pl.semaphore_signal(sem, inc=1, device_id={axis: index}, device_id_type=pl.DeviceIdType.MESH)

    @pl.when(my_layer < layers - 1)
    def _():
        for k in range(1, layers):
            for part in range(SLICES):
                greet(barrier, "own", lax.rem(my_layer + k, layers) * SLICES + part)

    @pl.when(my_layer == layers - 1)
    def _():
        for part in range(SLICES):
            greet(barrier, "own", part)

    @pl.when(jnp.logical_not(is_inner))
    def _():
        for part in range(1, SLICES):
            greet(barrier, "own", my_layer * SLICES + lax.rem(my_slice + part, SLICES))

    for k in range(1, rep_n):
        greet(barrier, "rep", lax.rem(rep + k, rep_n))
    for pool, start, sem in ((pool_a, 0, pool_sem.at[0]), (pool_b, early, pool_sem.at[1])):
        for p in range(PIECES):
            here = pl.ds(p * (rows // PIECES), rows // PIECES)
            pltpu.make_async_copy(pool_ref.at[here, start:start + pool.shape[1]], pool.at[here], sem).start()

    def load_wait(pool, sem):
        pltpu.make_async_copy(pool_ref.at[:, 0:pool.shape[1]], pool.at[pl.ds(0, rows)], sem).wait()

    pool_a[rows] = jnp.zeros(pool_a.shape[1:], pool_a.dtype)
    pool_b[rows] = jnp.zeros(pool_b.shape[1:], pool_b.dtype)
    pltpu.make_async_copy(sel_v, sel_v, sel_sem).wait()
    filled = fill_slots(live_ref[0], sel_v[0], sel_v[1], table, layers, cap, rows)
    to_scalars = pltpu.make_async_copy(table, slots, table_sem)
    to_scalars.start()
    last = partner_layer(my_layer, layers, layers // 2)
    place = lax.broadcasted_iota(jnp.int32, filled.shape, 1)
    first_rows = []
    for c in range(cap):
        row = jnp.sum(jnp.where(place == last * cap + c, filled, 0.0)).astype(jnp.int32)
        first_rows.append(jnp.minimum(jnp.maximum(row, 0), rows))
    load_wait(pool_a, pool_sem.at[0])

    def row_of(slot):
        return jnp.minimum(jnp.maximum(slots[0, slot], 0), rows)

    def layer_peak(layer, carry):
        best = [jnp.zeros(pool.shape[1:], pool.dtype) for pool in (pool_a, pool_b)]
        for c in range(cap):
            row = row_of(layer * cap + c)
            best = [jnp.maximum(b, jnp.abs(pool[row])) for b, pool in zip(best, (pool_a, pool_b))]
        tops = [jnp.max(b.astype(f32), axis=0, keepdims=True) for b in best]
        top = jnp.maximum(tops[0], tops[1])
        for part in range(SLICES):
            pk_send[layer * SLICES + part] = top[:, part * half:(part + 1) * half]
        return carry

    def own_copy(src, dst, s_sem, r_sem, peer):
        return pltpu.make_async_remote_copy(
            src_ref=src, dst_ref=dst, send_sem=s_sem, recv_sem=r_sem,
            device_id={"own": peer}, device_id_type=pl.DeviceIdType.MESH)

    def rep_copy(src, dst, r_sem, peer):
        return pltpu.make_async_remote_copy(
            src_ref=src, dst_ref=dst, send_sem=small_send, recv_sem=r_sem,
            device_id={"rep": peer}, device_id_type=pl.DeviceIdType.MESH)

    def rep_share(table, r_sem):
        for k in range(1, rep_n):
            rep_copy(table.at[rep], table.at[rep], r_sem, lax.rem(rep + k, rep_n)).start()

    def arrived(dst, count, r_sem):
        own_copy(dst.at[pl.ds(0, count)], dst.at[pl.ds(0, count)], small_send, r_sem, lax.rem(me + 1, own_n)).wait_recv()

    eighth = loops // 8
    raw = ((0, eighth), (eighth, eighth // 2))
    coded = (eighth + eighth // 2, loops - eighth - eighth // 2)
    early_cols = ((0, eighth), (eighth, 5 * eighth))
    held = (6 * eighth, loops - 6 * eighth)
    all_cols = (0, loops)

    def block_copy(peer, landing, cols, into, r_sem):
        lanes = pl.ds(cols[0] * period, cols[1] * period)
        return own_copy(send.at[peer, :, lanes], into.at[landing, :, lanes], send_sem, r_sem, peer)

    def flatten_layer(layer, cols, known=None):
        start, count = cols
        ranges = []
        for pool, begin in ((pool_a, 0), (pool_b, early)):
            t0, t1 = max(start * group, begin), min((start + count) * group, begin + pool.shape[1])
            if t0 < t1:
                ranges.append((pool, begin, t0, t1))
        for c in range(cap):
            row = known[c] if known else row_of(layer * cap + c)
            for pool, begin, t0, t1 in ranges:
                block = pool[row, t0 - begin:t1 - begin, :].astype(f32)
                for q in range(tiles):
                    lo, hi = q * LANES, min(width, (q + 1) * LANES)
                    stage[q, c * tokens + t0:c * tokens + t1, 0:hi - lo] = block[:, lo:hi]

        def flatten(i, carry):
            rows_of = [
                jnp.concatenate(
                    [stage[q, pl.ds(i * group + j, cap, stride=tokens), :] for q in range(tiles)], axis=1)
                for j in range(group)
            ]
            for part in range(SLICES):
                joined = jnp.concatenate([r[:, part * half:(part + 1) * half] for r in rows_of], axis=1)
                at = pl.multiple_of(i * period, period)
                send[layer * SLICES + part, :, pl.ds(at, period)] = joined.astype(send.dtype)
            return carry

        lax.fori_loop(start, start + count, flatten, 0)

    def owner(layer, part):
        return layer * SLICES + lax.rem(my_slice + part, SLICES)

    across_first = list(range(1, SLICES)) + [0]
    order = [k for k in range(1, layers) if k != layers // 2]
    to_layer = [partner_layer(my_layer, layers, k) for k in order]
    from_layer = [partner_layer(my_layer, layers, layers - k) for k in order]
    mine_sem, last_sem, raw_sem = (recv_sem.at[layers - 2 + i] for i in range(3))
    pk_sem, pr_sem, st_sem, pe_sem, er_sem = (small_recv.at[i] for i in range(5))

    def send_blocks(i, cols):
        for part in across_first:
            block_copy(owner(to_layer[i], part), me, cols, recv, recv_sem.at[i]).start()

    def send_last(cols, into, r_sem):
        for part in across_first:
            block_copy(owner(last, part), me, cols, into, r_sem).start()

    flatten_layer(last, raw[0], first_rows)
    pl.semaphore_wait(barrier, own_n - 1 + rep_n - 1 - jnp.where(is_inner, 2 * SLICES - 1, 0))
    send_last(raw[0], recv, raw_sem)

    @pl.when(my_layer == 0)
    def _():
        for layer in range(1, layers - 1):
            greet(late_sem, "own", layer * SLICES + my_slice)

    to_scalars.wait()
    flatten_layer(last, raw[1])
    send_last(raw[1], recv, raw_sem)
    load_wait(pool_b, pool_sem.at[1])
    lax.fori_loop(0, layers, layer_peak, 0, unroll=4)
    flatten_layer(to_layer[0], early_cols[0])
    is_later = is_inner & (to_layer[0] == layers - 1)

    @pl.when(jnp.logical_not(is_later))
    def _():
        send_blocks(0, early_cols[0])

    flatten_layer(to_layer[0], early_cols[1])

    @pl.when(is_inner)
    def _():
        pl.semaphore_wait(late_sem, 1)

    for k in range(1, own_n):
        peer = lax.rem(me + k, own_n)
        own_copy(pk_send.at[peer], pk_recv.at[me], small_send, pk_sem, peer).start()

    @pl.when(is_later)
    def _():
        send_blocks(0, early_cols[0])

    send_blocks(0, early_cols[1])
    flatten_layer(to_layer[0], held)
    for i in range(1, layers - 2):
        flatten_layer(to_layer[i], all_cols)
    flatten_layer(last, coded)

    arrived(pk_recv, own_n - 1, pk_sem)
    best = pk_send[me]
    for k in range(1, own_n):
        best = jnp.maximum(best, pk_recv[lax.rem(me + k, own_n)])
    pk_rep[rep] = best
    rep_share(pk_rep, pr_sem)
    flatten_layer(my_layer, all_cols)
    arrived(pk_rep, rep_n - 1, pr_sem)
    for k in range(1, rep_n):
        best = jnp.maximum(best, pk_rep[lax.rem(rep + k, rep_n)])

    step = headroom * jnp.maximum(best, 1.0) / 127.0
    steps_ref[...] = step
    mine[...] = step
    for part in across_first:
        own_copy(mine, st_recv.at[me], small_send, st_sem, owner(last, part)).start()
    for i in range(1, layers - 2):
        send_blocks(i, all_cols)
    send_blocks(0, held)
    for part in range(1, SLICES):
        block_copy(owner(my_layer, part), me, all_cols, recv, mine_sem).start()

    def wide(row):
        return jnp.broadcast_to(jnp.concatenate([row] * group, axis=1), (cap, period))

    def encode(source, target, src, one_step, total, cols=all_cols):
        step_wide = wide(one_step)
        inv_wide = wide(1.0 / one_step)

        def one(i, total):
            lanes = pl.ds(pl.multiple_of(i * period, period), period)
            x = source[src, :, lanes].astype(f32)
            y = jnp.clip(x * inv_wide, -127.0, 127.0).astype(codes_ref.dtype)
            target[src, :, lanes] = y
            diff = x - y.astype(f32) * step_wide
            return total + diff * diff
        return lax.fori_loop(cols[0], cols[0] + cols[1], one, total)

    def fold(total):
        row = jnp.sum(total, axis=0, keepdims=True)
        folded = row[:, :half]
        for j in range(1, group):
            folded = folded + row[:, j * half:(j + 1) * half]
        return folded

    def blocks_arrived(count, r_sem, n_loops=loops):
        some = recv.at[pl.ds(0, count), :, pl.ds(0, n_loops * period)]
        own_copy(some, some, small_send, r_sem, lax.rem(me + 1, own_n)).wait_recv()

    zero = jnp.zeros((cap, period), f32)
    codes_at = codes_ref.at[0, 0]
    total = encode(send, codes_at, me, step, zero)

    arrived(st_recv, SLICES, st_sem)
    for part in across_first:
        peer = owner(last, part)
        pe_send[peer] = fold(encode(send, send, peer, st_recv[peer], zero, coded))
        own_copy(pe_send.at[peer], pe_recv.at[me], small_send, pe_sem, peer).start()
    send_last(coded, codes_at, last_sem)

    blocks_arrived(SLICES, raw_sem, coded[0])
    for part in across_first:
        total = encode(recv, codes_at, owner(last, part), step, total, (0, coded[0]))
    blocks_arrived(SLICES, recv_sem.at[0])
    for part in across_first:
        total = encode(recv, codes_at, owner(from_layer[0], part), step, total)
    blocks_arrived(SLICES - 1, mine_sem)
    for part in range(1, SLICES):
        total = encode(recv, codes_at, owner(my_layer, part), step, total)
    for i in range(1, layers - 2):
        blocks_arrived(SLICES, recv_sem.at[i])
        for part in across_first:
            total = encode(recv, codes_at, owner(from_layer[i], part), step, total)

    error = fold(total)
    arrived(pe_recv, SLICES, pe_sem)
    for part in across_first:
        error = error + pe_recv[owner(last, part)]
    er_rep[rep] = error
    rep_share(er_rep, er_sem)
    arrived(er_rep, rep_n - 1, er_sem)
    whole = er_rep[0]
    for k in range(1, rep_n):
        whole = whole + er_rep[k]
    err_ref[...] = whole / (step * step * denominator)

    peer = lax.rem(me + 1, own_n)
    sent = own_n - 1 + 2 * (rep_n - 1) + 2 * SLICES
    many = pk_send.at[pl.ds(0, sent)]
    own_copy(many, many, small_send, last_sem, peer).wait_send()
    own_copy(send.at[pl.ds(0, own_n - 1)], recv.at[pl.ds(0, own_n - 1)], send_sem, last_sem, peer).wait_send()
    blocks_arrived(SLICES, last_sem, coded[1])


def write_out(codes_v, steps_v, err_v, codes_ref, steps_ref, err_ref, sem, small_sem):
    own_n = codes_v.shape[2]
    for src in range(own_n):
        pltpu.make_async_copy(codes_v.at[0, 0, src], codes_ref.at[0, 0, src], sem).start()
    smalls = [pltpu.make_async_copy(steps_v, steps_ref, small_sem.at[0]),
              pltpu.make_async_copy(err_v, err_ref, small_sem.at[1])]
    for small in smalls:
        small.start()
    pltpu.make_async_copy(codes_v, codes_ref, sem).wait()
    for small in smalls:
        small.wait()


def body(block_pool, sel_index, sel_layer, counts):
    own_n = lax.axis_size("own")
    rep_n = lax.axis_size("rep")
    cap = sel_index.shape[0] // 4
    rows, tokens, width = block_pool.shape
    n_select = sel_index.shape[0]
    half = width // SLICES
    flat = tokens * half
    layers = own_n // SLICES
    f32, i32 = jnp.float32, jnp.int32
    dma = pltpu.SemaphoreType.DMA
    dtype = block_pool.dtype

    def row(n):
        return pltpu.VMEM((n, 1, half), f32)

    hbm = pl.BlockSpec(memory_space=pltpu.HBM)
    vmem = pl.BlockSpec(memory_space=pltpu.VMEM)
    codes, steps, err = pl.pallas_call(
        functools.partial(kernel, own_n, rep_n, cap),
        out_shape=(
            pltpu.VMEM((1, 1, own_n, cap, flat), dtype),
            pltpu.VMEM((1, half), f32),
            pltpu.VMEM((1, half), f32),
        ),
        in_specs=[pl.BlockSpec(memory_space=pltpu.SMEM)] + [hbm] * 3,
        out_specs=(vmem,) * 3,
        scratch_shapes=[
            pltpu.VMEM((2, 1, n_select), i32),
            pltpu.VMEM((1, pl.cdiv(layers * cap, LANES) * LANES), i32),
            pltpu.SMEM((1, pl.cdiv(layers * cap, LANES) * LANES), i32),
            pltpu.VMEM((rows + 1, tokens // 4, width), dtype),
            pltpu.VMEM((rows + 1, tokens - tokens // 4, width), dtype),
            pltpu.VMEM((pl.cdiv(width, LANES), cap * tokens, LANES), f32),
            pltpu.VMEM((own_n, cap, flat), dtype),
            pltpu.VMEM((own_n, cap, flat), dtype),
            row(own_n + 2 * rep_n + 2 * SLICES), row(own_n), row(rep_n),
            row(own_n), row(own_n), row(own_n), row(rep_n), pltpu.VMEM((1, half), f32),
            dma, dma, dma((2,)), dma, dma((layers + 1,)), dma, dma((5,)), pltpu.SemaphoreType.REGULAR,
        ],
        compiler_params=pltpu.CompilerParams(
            collective_id=0, has_side_effects=True, vmem_limit_bytes=(63 * 1024 * 1024 - own_n * cap * flat * 2)),
        name="latent_code",
    )(counts, sel_index[None], sel_layer[None], block_pool)
    return pl.pallas_call(
        write_out,
        out_shape=tuple(jax.ShapeDtypeStruct(x.shape, x.dtype) for x in (codes, steps, err)),
        in_specs=[vmem] * 3,
        out_specs=(hbm, hbm, hbm),
        scratch_shapes=[dma, dma((2,))],
        compiler_params=pltpu.CompilerParams(vmem_limit_bytes=4 * 1024 * 1024),
        name="write_out",
    )(codes, steps, err)


def solution(mesh):
    return jax.shard_map(
        body,
        mesh=mesh,
        in_specs=(
            P(("own", "rep"), None, None),
            P(("own", "rep")),
            P(("own", "rep")),
            P(("own", "rep")),
        ),
        out_specs=(P("own", "rep", None, None, None), P("own", None), P("own", None)),
        check_vma=False,
    )
```

```python
import functools
import math

import jax
import jax.numpy as jnp
from jax import lax
from jax.experimental import pallas as pl
from jax.experimental.pallas import tpu as pltpu
from jax.sharding import PartitionSpec as P

SLICES = 2
LANES = 128
PIECES = 8
headroom = 0.5


def ring_place(layer, layers):
    odd = layer % 2
    return odd * ((layer + 1) // 2) + (1 - odd) * lax.rem(layers - layer // 2, layers)


def ring_layer(place, layers):
    near = jnp.maximum(2 * place - 1, 0)
    return jnp.where(place <= layers // 2, near, 2 * (layers - place))


def partner_layer(my_layer, layers, k):
    return ring_layer(lax.rem(ring_place(my_layer, layers) + k, layers), layers)


def fill_slots(live, index_row, layer_row, table, layers, cap, empty):
    n_select = index_row.shape[1]
    is_live = lax.broadcasted_iota(jnp.int32, (1, n_select), 1) < live
    before = lax.broadcasted_iota(jnp.int32, (n_select, n_select), 0)
    after = lax.broadcasted_iota(jnp.int32, (n_select, n_select), 1)
    earlier = jnp.where(before < after, 1.0, 0.0)
    wanted = lax.broadcasted_iota(jnp.int32, (layers, n_select), 0)
    matches = jnp.where((layer_row == wanted) & is_live, 1.0, 0.0)
    ranking = jnp.dot(matches, earlier, preferred_element_type=jnp.float32)
    slot = lax.broadcasted_iota(jnp.int32, (cap, n_select), 0).astype(jnp.float32)
    shifted = index_row.astype(jnp.float32) - float(empty)
    place = lax.broadcasted_iota(jnp.int32, (cap, table.shape[1]), 1)
    spread = jnp.zeros((cap, table.shape[1]), jnp.float32)
    for layer in range(layers):
        hit = (ranking[layer:layer + 1] == slot) & (matches[layer:layer + 1] > 0.5)
        found = jnp.sum(jnp.where(hit, shifted, 0.0), axis=1, keepdims=True) + float(empty)
        here = place == layer * cap + lax.broadcasted_iota(jnp.int32, place.shape, 0)
        spread = spread + jnp.where(here, found, 0.0)
    row = jnp.sum(spread, axis=0, keepdims=True)
    table[...] = row.astype(jnp.int32)
    return row


def kernel(own_n, rep_n, cap, live_ref, index_hbm, layer_hbm, pool_ref, codes_ref, steps_ref, err_ref,
           sel_v, table, slots, pool_a, pool_b, stage, send, recv, pk_send, pk_recv, pk_rep,
           st_recv, pe_send, pe_recv, er_rep, mine,
           sel_sem, table_sem, pool_sem, send_sem, recv_sem, small_send, small_recv, late_sem):
    rows, tokens, width = pool_ref.shape
    half = width // SLICES
    group = LANES // math.gcd(half, LANES)
    period = group * half
    loops = tokens // group
    layers = own_n // SLICES
    me = lax.axis_index("own")
    rep = lax.axis_index("rep")
    my_layer = me // SLICES
    my_slice = me % SLICES
    tiles = stage.shape[0]
    denominator = float(own_n * rep_n * cap * tokens)
    f32 = jnp.float32
    early = pool_a.shape[1]

    sels = [pltpu.make_async_copy(index_hbm, sel_v.at[0], sel_sem),
            pltpu.make_async_copy(layer_hbm, sel_v.at[1], sel_sem)]
    for sel in sels:
        sel.start()
    barrier = pltpu.get_barrier_semaphore()
    is_inner = (my_layer > 0) & (my_layer < layers - 1)

    def greet(sem, axis, index):
        pl.semaphore_signal(sem, inc=1, device_id={axis: index}, device_id_type=pl.DeviceIdType.MESH)

    @pl.when(my_layer < layers - 1)
    def _():
        for k in range(1, layers):
            for part in range(SLICES):
                greet(barrier, "own", lax.rem(my_layer + k, layers) * SLICES + part)

    @pl.when(my_layer == layers - 1)
    def _():
        for part in range(SLICES):
            greet(barrier, "own", part)

    @pl.when(jnp.logical_not(is_inner))
    def _():
        for part in range(1, SLICES):
            greet(barrier, "own", my_layer * SLICES + lax.rem(my_slice + part, SLICES))

    for k in range(1, rep_n):
        greet(barrier, "rep", lax.rem(rep + k, rep_n))
    for pool, start, sem in ((pool_a, 0, pool_sem.at[0]), (pool_b, early, pool_sem.at[1])):
        for p in range(PIECES):
            here = pl.ds(p * (rows // PIECES), rows // PIECES)
            pltpu.make_async_copy(pool_ref.at[here, start:start + pool.shape[1]], pool.at[here], sem).start()

    def load_wait(pool, sem):
        pltpu.make_async_copy(pool_ref.at[:, 0:pool.shape[1]], pool.at[pl.ds(0, rows)], sem).wait()

    pool_a[rows] = jnp.zeros(pool_a.shape[1:], pool_a.dtype)
    pool_b[rows] = jnp.zeros(pool_b.shape[1:], pool_b.dtype)
    pltpu.make_async_copy(sel_v, sel_v, sel_sem).wait()
    filled = fill_slots(live_ref[0], sel_v[0], sel_v[1], table, layers, cap, rows)
    to_scalars = pltpu.make_async_copy(table, slots, table_sem)
    to_scalars.start()
    last = partner_layer(my_layer, layers, layers // 2)
    place = lax.broadcasted_iota(jnp.int32, filled.shape, 1)
    first_rows = []
    for c in range(cap):
        row = jnp.sum(jnp.where(place == last * cap + c, filled, 0.0)).astype(jnp.int32)
        first_rows.append(jnp.minimum(jnp.maximum(row, 0), rows))
    load_wait(pool_a, pool_sem.at[0])

    def row_of(slot):
        return jnp.minimum(jnp.maximum(slots[0, slot], 0), rows)

    def layer_peak(layer, carry):
        best = [jnp.zeros(pool.shape[1:], pool.dtype) for pool in (pool_a, pool_b)]
        for c in range(cap):
            row = row_of(layer * cap + c)
            best = [jnp.maximum(b, jnp.abs(pool[row])) for b, pool in zip(best, (pool_a, pool_b))]
        tops = [jnp.max(b.astype(f32), axis=0, keepdims=True) for b in best]
        top = jnp.maximum(tops[0], tops[1])
        for part in range(SLICES):
            pk_send[layer * SLICES + part] = top[:, part * half:(part + 1) * half]
        return carry

    def own_copy(src, dst, s_sem, r_sem, peer):
        return pltpu.make_async_remote_copy(
            src_ref=src, dst_ref=dst, send_sem=s_sem, recv_sem=r_sem,
            device_id={"own": peer}, device_id_type=pl.DeviceIdType.MESH)

    def rep_copy(src, dst, r_sem, peer):
        return pltpu.make_async_remote_copy(
            src_ref=src, dst_ref=dst, send_sem=small_send, recv_sem=r_sem,
            device_id={"rep": peer}, device_id_type=pl.DeviceIdType.MESH)

    def rep_share(table, r_sem):
        for k in range(1, rep_n):
            rep_copy(table.at[rep], table.at[rep], r_sem, lax.rem(rep + k, rep_n)).start()

    def arrived(dst, count, r_sem):
        own_copy(dst.at[pl.ds(0, count)], dst.at[pl.ds(0, count)], small_send, r_sem, lax.rem(me + 1, own_n)).wait_recv()

    eighth = loops // 8
    raw = ((0, eighth), (eighth, eighth // 2))
    coded = (eighth + eighth // 2, loops - eighth - eighth // 2)
    early_cols = ((0, eighth), (eighth, 5 * eighth))
    held = (6 * eighth, loops - 6 * eighth)
    all_cols = (0, loops)

    def block_copy(peer, landing, cols, into, r_sem):
        lanes = pl.ds(cols[0] * period, cols[1] * period)
        return own_copy(send.at[peer, :, lanes], into.at[landing, :, lanes], send_sem, r_sem, peer)

    def flatten_layer(layer, cols, known=None):
        start, count = cols
        ranges = []
        for pool, begin in ((pool_a, 0), (pool_b, early)):
            t0, t1 = max(start * group, begin), min((start + count) * group, begin + pool.shape[1])
            if t0 < t1:
                ranges.append((pool, begin, t0, t1))
        for c in range(cap):
            row = known[c] if known else row_of(layer * cap + c)
            for pool, begin, t0, t1 in ranges:
                block = pool[row, t0 - begin:t1 - begin, :].astype(f32)
                for q in range(tiles):
                    lo, hi = q * LANES, min(width, (q + 1) * LANES)
                    stage[q, c * tokens + t0:c * tokens + t1, 0:hi - lo] = block[:, lo:hi]

        def flatten(i, carry):
            rows_of = [
                jnp.concatenate(
                    [stage[q, pl.ds(i * group + j, cap, stride=tokens), :] for q in range(tiles)], axis=1)
                for j in range(group)
            ]
            for part in range(SLICES):
                joined = jnp.concatenate([r[:, part * half:(part + 1) * half] for r in rows_of], axis=1)
                at = pl.multiple_of(i * period, period)
                send[layer * SLICES + part, :, pl.ds(at, period)] = joined.astype(send.dtype)
            return carry

        lax.fori_loop(start, start + count, flatten, 0)

    def owner(layer, part):
        return layer * SLICES + lax.rem(my_slice + part, SLICES)

    across_first = list(range(1, SLICES)) + [0]
    order = [k for k in range(1, layers) if k != layers // 2]
    to_layer = [partner_layer(my_layer, layers, k) for k in order]
    from_layer = [partner_layer(my_layer, layers, layers - k) for k in order]
    mine_sem, last_sem, raw_sem = (recv_sem.at[layers - 2 + i] for i in range(3))
    pk_sem, pr_sem, st_sem, pe_sem, er_sem = (small_recv.at[i] for i in range(5))

    def send_blocks(i, cols):
        for part in (across_first if i else across_first[::-1]):
            block_copy(owner(to_layer[i], part), me, cols, recv, recv_sem.at[i]).start()

    def send_last(cols, into, r_sem):
        for part in across_first:
            block_copy(owner(last, part), me, cols, into, r_sem).start()

    flatten_layer(last, raw[0], first_rows)
    pl.semaphore_wait(barrier, own_n - 1 + rep_n - 1 - jnp.where(is_inner, 2 * SLICES - 1, 0))
    send_last(raw[0], recv, raw_sem)

    @pl.when(my_layer == 0)
    def _():
        for layer in range(1, layers - 1):
            greet(late_sem, "own", layer * SLICES + my_slice)

    to_scalars.wait()
    flatten_layer(last, raw[1])
    send_last(raw[1], recv, raw_sem)
    load_wait(pool_b, pool_sem.at[1])
    lax.fori_loop(0, layers, layer_peak, 0, unroll=4)
    flatten_layer(to_layer[0], early_cols[0])
    is_later = is_inner & (to_layer[0] == layers - 1)

    @pl.when(jnp.logical_not(is_later))
    def _():
        send_blocks(0, early_cols[0])

    flatten_layer(to_layer[0], early_cols[1])

    @pl.when(is_inner)
    def _():
        pl.semaphore_wait(late_sem, 1)

    for k in range(1, own_n):
        peer = lax.rem(me + k, own_n)
        own_copy(pk_send.at[peer], pk_recv.at[me], small_send, pk_sem, peer).start()

    @pl.when(is_later)
    def _():
        send_blocks(0, early_cols[0])

    send_blocks(0, early_cols[1])
    flatten_layer(to_layer[0], held)
    for i in range(1, layers - 2):
        flatten_layer(to_layer[i], all_cols)
    flatten_layer(last, coded)

    arrived(pk_recv, own_n - 1, pk_sem)
    best = pk_send[me]
    for k in range(1, own_n):
        best = jnp.maximum(best, pk_recv[lax.rem(me + k, own_n)])
    pk_rep[rep] = best
    rep_share(pk_rep, pr_sem)
    flatten_layer(my_layer, all_cols)
    arrived(pk_rep, rep_n - 1, pr_sem)
    for k in range(1, rep_n):
        best = jnp.maximum(best, pk_rep[lax.rem(rep + k, rep_n)])

    step = headroom * jnp.maximum(best, 1.0) / 127.0
    steps_ref[...] = step
    mine[...] = step
    for part in across_first:
        own_copy(mine, st_recv.at[me], small_send, st_sem, owner(last, part)).start()
    for i in range(1, layers - 2):
        send_blocks(i, all_cols)
    send_blocks(0, held)
    for part in range(1, SLICES):
        block_copy(owner(my_layer, part), me, all_cols, recv, mine_sem).start()

    def wide(row):
        return jnp.broadcast_to(jnp.concatenate([row] * group, axis=1), (cap, period))

    def encode(source, target, src, one_step, total, cols=all_cols):
        step_wide = wide(one_step)
        inv_wide = wide(1.0 / one_step)

        def one(i, total):
            lanes = pl.ds(pl.multiple_of(i * period, period), period)
            x = source[src, :, lanes].astype(f32)
            y = jnp.clip(x * inv_wide, -127.0, 127.0).astype(codes_ref.dtype)
            target[src, :, lanes] = y
            diff = x - y.astype(f32) * step_wide
            return total + diff * diff
        return lax.fori_loop(cols[0], cols[0] + cols[1], one, total)

    def fold(total):
        row = jnp.sum(total, axis=0, keepdims=True)
        folded = row[:, :half]
        for j in range(1, group):
            folded = folded + row[:, j * half:(j + 1) * half]
        return folded

    def blocks_arrived(count, r_sem, n_loops=loops):
        some = recv.at[pl.ds(0, count), :, pl.ds(0, n_loops * period)]
        own_copy(some, some, small_send, r_sem, lax.rem(me + 1, own_n)).wait_recv()

    zero = jnp.zeros((cap, period), f32)
    codes_at = codes_ref.at[0, 0]
    total = encode(send, codes_at, me, step, zero)

    arrived(st_recv, SLICES, st_sem)
    for part in across_first:
        peer = owner(last, part)
        pe_send[peer] = fold(encode(send, send, peer, st_recv[peer], zero, coded))
        own_copy(pe_send.at[peer], pe_recv.at[me], small_send, pe_sem, peer).start()
    send_last(coded, codes_at, last_sem)

    blocks_arrived(SLICES, raw_sem, coded[0])
    for part in across_first:
        total = encode(recv, codes_at, owner(last, part), step, total, (0, coded[0]))
    blocks_arrived(SLICES, recv_sem.at[0])
    for part in across_first:
        total = encode(recv, codes_at, owner(from_layer[0], part), step, total)
    blocks_arrived(SLICES - 1, mine_sem)
    for part in range(1, SLICES):
        total = encode(recv, codes_at, owner(my_layer, part), step, total)
    for i in range(1, layers - 2):
        blocks_arrived(SLICES, recv_sem.at[i])
        for part in across_first:
            total = encode(recv, codes_at, owner(from_layer[i], part), step, total)

    error = fold(total)
    arrived(pe_recv, SLICES, pe_sem)
    for part in across_first:
        error = error + pe_recv[owner(last, part)]
    er_rep[rep] = error
    rep_share(er_rep, er_sem)
    arrived(er_rep, rep_n - 1, er_sem)
    whole = er_rep[0]
    for k in range(1, rep_n):
        whole = whole + er_rep[k]
    err_ref[...] = whole / (step * step * denominator)

    peer = lax.rem(me + 1, own_n)
    sent = own_n - 1 + 2 * (rep_n - 1) + 2 * SLICES
    many = pk_send.at[pl.ds(0, sent)]
    own_copy(many, many, small_send, last_sem, peer).wait_send()
    own_copy(send.at[pl.ds(0, own_n - 1)], recv.at[pl.ds(0, own_n - 1)], send_sem, last_sem, peer).wait_send()
    blocks_arrived(SLICES, last_sem, coded[1])


def write_out(codes_v, steps_v, err_v, codes_ref, steps_ref, err_ref, sem, small_sem):
    own_n = codes_v.shape[2]
    for src in range(own_n):
        pltpu.make_async_copy(codes_v.at[0, 0, src], codes_ref.at[0, 0, src], sem).start()
    smalls = [pltpu.make_async_copy(steps_v, steps_ref, small_sem.at[0]),
              pltpu.make_async_copy(err_v, err_ref, small_sem.at[1])]
    for small in smalls:
        small.start()
    pltpu.make_async_copy(codes_v, codes_ref, sem).wait()
    for small in smalls:
        small.wait()


def body(block_pool, sel_index, sel_layer, counts):
    own_n = lax.axis_size("own")
    rep_n = lax.axis_size("rep")
    cap = sel_index.shape[0] // 4
    rows, tokens, width = block_pool.shape
    n_select = sel_index.shape[0]
    half = width // SLICES
    flat = tokens * half
    layers = own_n // SLICES
    f32, i32 = jnp.float32, jnp.int32
    dma = pltpu.SemaphoreType.DMA
    dtype = block_pool.dtype

    def row(n):
        return pltpu.VMEM((n, 1, half), f32)

    hbm = pl.BlockSpec(memory_space=pltpu.HBM)
    vmem = pl.BlockSpec(memory_space=pltpu.VMEM)
    codes, steps, err = pl.pallas_call(
        functools.partial(kernel, own_n, rep_n, cap),
        out_shape=(
            pltpu.VMEM((1, 1, own_n, cap, flat), dtype),
            pltpu.VMEM((1, half), f32),
            pltpu.VMEM((1, half), f32),
        ),
        in_specs=[pl.BlockSpec(memory_space=pltpu.SMEM)] + [hbm] * 3,
        out_specs=(vmem,) * 3,
        scratch_shapes=[
            pltpu.VMEM((2, 1, n_select), i32),
            pltpu.VMEM((1, pl.cdiv(layers * cap, LANES) * LANES), i32),
            pltpu.SMEM((1, pl.cdiv(layers * cap, LANES) * LANES), i32),
            pltpu.VMEM((rows + 1, tokens // 4, width), dtype),
            pltpu.VMEM((rows + 1, tokens - tokens // 4, width), dtype),
            pltpu.VMEM((pl.cdiv(width, LANES), cap * tokens, LANES), f32),
            pltpu.VMEM((own_n, cap, flat), dtype),
            pltpu.VMEM((own_n, cap, flat), dtype),
            row(own_n + 2 * rep_n + 2 * SLICES), row(own_n), row(rep_n),
            row(own_n), row(own_n), row(own_n), row(rep_n), pltpu.VMEM((1, half), f32),
            dma, dma, dma((2,)), dma, dma((layers + 1,)), dma, dma((5,)), pltpu.SemaphoreType.REGULAR,
        ],
        compiler_params=pltpu.CompilerParams(
            collective_id=0, has_side_effects=True, vmem_limit_bytes=(63 * 1024 * 1024 - own_n * cap * flat * 2)),
        name="latent_code",
    )(counts, sel_index[None], sel_layer[None], block_pool)
    return pl.pallas_call(
        write_out,
        out_shape=tuple(jax.ShapeDtypeStruct(x.shape, x.dtype) for x in (codes, steps, err)),
        in_specs=[vmem] * 3,
        out_specs=(hbm, hbm, hbm),
        scratch_shapes=[dma, dma((2,))],
        compiler_params=pltpu.CompilerParams(vmem_limit_bytes=4 * 1024 * 1024),
        name="write_out",
    )(codes, steps, err)


def solution(mesh):
    return jax.shard_map(
        body,
        mesh=mesh,
        in_specs=(
            P(("own", "rep"), None, None),
            P(("own", "rep")),
            P(("own", "rep")),
            P(("own", "rep")),
        ),
        out_specs=(P("own", "rep", None, None, None), P("own", None), P("own", None)),
        check_vma=False,
    )
```
